32 devices in a mesh: fsdp: 8 (over y, x, core), model: 4 (over z).
Axes of the slice: x: 2, y: 2, z: 4, core: 2. Of those that a mesh axis runs over, the one named last changes fastest.
Arguments:
- w_query: float32 [4096, 4096], P('fsdp', 'model'), may hold values from -0.125 to 0.125
- first_query: float32 [4096, 4096], P('fsdp', 'model'), may hold values from -0.09375 to 0.09375
- second_query: float32 [4096, 4096], P('fsdp', 'model'), may hold values from -0.09375 to 0.09375
- w_key: float32 [4096, 4096], P('fsdp', 'model'), may hold values from -0.125 to 0.125
- first_key: float32 [4096, 4096], P('fsdp', 'model'), may hold values from -0.09375 to 0.09375
- second_key: float32 [4096, 4096], P('fsdp', 'model'), may hold values from -0.09375 to 0.09375
- w_value: float32 [4096, 4096], P('fsdp', 'model'), may hold values from -0.125 to 0.125
- first_value: float32 [4096, 4096], P('fsdp', 'model'), may hold values from -0.09375 to 0.09375
- second_value: float32 [4096, 4096], P('fsdp', 'model'), may hold values from -0.09375 to 0.09375
- norm_gain: float32 [4096], P('fsdp'), may hold values from 0.25 to 1.75
Outputs:
- ready_query: bfloat16 [4096, 4096], P(None, 'model')
- ready_key: bfloat16 [4096, 4096], P(None, 'model')
- ready_value: bfloat16 [4096, 4096], P(None, 'model')
- factor_query: float32 [4096], P('model')
- factor_key: float32 [4096], P('model')
- factor_value: float32 [4096], P('model')
The draws below stay inside these ranges and needn't reach their ends.
All inputs are finite; a program needn't handle non-finite values. Where the reference program divides by a largest or mean magnitude, that divisor is 1e-20 or more.
Results may differ from the reference program's by a relative error of at most 0.001.
Values may be sent and summed in bfloat16 or wider, within the bound.
A program may use at most 128 MiB of HBM per device.

```python
import jax
import jax.numpy as jnp

D_MODEL = 4096
Q_DIM = 4096
KV_DIM = 4096


def strengthened(values, own_key, source, target, shards_of, factor):
    def block_of(axis_at):
        return (jnp.arange(values.shape[axis_at]) // (values.shape[axis_at] // shards_of)).reshape((-1,) + (1,) * (values.ndim - 1 - axis_at))

    one_side = jax.random.permutation(own_key, shards_of)[block_of(target)]
    far = (block_of(target) + shards_of // 2) % shards_of
    return jnp.where((block_of(source) == one_side) | (block_of(source) == far), factor * values, values)


def levels(key, extent, cuts, low, top_value):
    gain, own = 1.0, jax.random.fold_in(key, 6)
    for position, parts in cuts:
        heights = jnp.exp(jax.random.uniform(jax.random.fold_in(own, position), (parts,), jnp.float32, low / len(cuts), top_value / len(cuts)))
        gain = gain * jnp.repeat(heights, extent[position] // parts).reshape([-1 if axis == position else 1 for axis in range(len(extent))])
    return gain


def centred(own_key, shape, deviation, most, split=(), kind=jnp.bfloat16):
    values = deviation * jax.random.normal(own_key, shape, jnp.float32)
    if split:
        values = values * levels(own_key, shape, split, -0.22, 0.18)
    return jnp.clip(values, -most, most).astype(kind)


def gaussian_with(key, extent, scale, most, pieces, heavy, kind=jnp.bfloat16):
    drawn = scale * jax.random.normal(key, extent, jnp.float32)
    if pieces:
        drawn = drawn * levels(key, extent, pieces, -0.22, 0.18)
    return jnp.clip(strengthened(drawn, jax.random.fold_in(key, 3), *heavy), -most, most).astype(kind)


def setup_inputs(seed: int = 0) -> dict:
    key_of = jax.random.split(jax.random.key(seed), 11)
    return {
        "w_query": gaussian_with(key_of[0], (D_MODEL, Q_DIM), D_MODEL ** -0.5, 0.125, ((0, 8), (1, 4)), (0, 1, 8, 2.0), jnp.float32),
        "first_query": centred(key_of[1], (D_MODEL, Q_DIM), D_MODEL ** -0.5, 0.09375, ((0, 8), (1, 4)), jnp.float32),
        "second_query": centred(key_of[2], (D_MODEL, Q_DIM), D_MODEL ** -0.5, 0.09375, ((0, 8), (1, 4)), jnp.float32),
        "w_key": gaussian_with(key_of[3], (D_MODEL, KV_DIM), D_MODEL ** -0.5, 0.125, ((0, 8), (1, 4)), (0, 1, 8, 2.0), jnp.float32),
        "first_key": centred(key_of[4], (D_MODEL, KV_DIM), D_MODEL ** -0.5, 0.09375, ((0, 8), (1, 4)), jnp.float32),
        "second_key": centred(key_of[5], (D_MODEL, KV_DIM), D_MODEL ** -0.5, 0.09375, ((0, 8), (1, 4)), jnp.float32),
        "w_value": gaussian_with(key_of[6], (D_MODEL, KV_DIM), D_MODEL ** -0.5, 0.125, ((0, 8), (1, 4)), (0, 1, 8, 2.0), jnp.float32),
        "first_value": centred(key_of[7], (D_MODEL, KV_DIM), D_MODEL ** -0.5, 0.09375, ((0, 8), (1, 4)), jnp.float32),
        "second_value": centred(key_of[8], (D_MODEL, KV_DIM), D_MODEL ** -0.5, 0.09375, ((0, 8), (1, 4)), jnp.float32),
        "norm_gain": jnp.clip(1.0 + 0.15 * jax.random.normal(key_of[9], (D_MODEL,), jnp.float32), 0.25, 1.75),
    }


learn_rate = 0.2
hold_rate = 0.9


def reference(w_query, first_query, second_query, w_key, first_key, second_key, w_value, first_value, second_value, norm_gain):
    hold_query = hold_rate * first_query + second_query
    latest_query = w_query - learn_rate * hold_query
    hold_key = hold_rate * first_key + second_key
    latest_key = w_key - learn_rate * hold_key
    hold_value = hold_rate * first_value + second_value
    latest_value = w_value - learn_rate * hold_value
    latest_gained_query = latest_query * norm_gain[:, None]
    latest_gained_key = latest_key * norm_gain[:, None]
    latest_gained_value = latest_value * norm_gain[:, None]
    factor_query = jnp.sum(jnp.abs(latest_gained_query), axis=0) / D_MODEL
    ready_query = (latest_gained_query / factor_query).astype(jnp.bfloat16)
    factor_key = jnp.sum(jnp.abs(latest_gained_key), axis=0) / D_MODEL
    ready_key = (latest_gained_key / factor_key).astype(jnp.bfloat16)
    factor_value = jnp.sum(jnp.abs(latest_gained_value), axis=0) / D_MODEL
    ready_value = (latest_gained_value / factor_value).astype(jnp.bfloat16)
    return ready_query, ready_key, ready_value, factor_query, factor_key, factor_value
```

```python
import functools
import math

import jax
import jax.numpy as jnp
from jax import lax
from jax.experimental import pallas as pl
from jax.experimental.pallas import tpu as pltpu
from jax.sharding import PartitionSpec as P

learn_rate = 0.2
hold_rate = 0.9
MESH = pl.DeviceIdType.MESH
UNITS = 8
PARTS = ((1, 2, 5), (8,), (4, 2, 1, 1))
STEP = 32
START = 1
AHEAD = 3
VMEM_BYTES = 67_043_328


def plain(
    w_query,
    first_query,
    second_query,
    w_key,
    first_key,
    second_key,
    w_value,
    first_value,
    second_value,
    norm_gain,
    rows,
):
    gained = []
    for w, first, second in (
        (w_query, first_query, second_query),
        (w_key, first_key, second_key),
        (w_value, first_value, second_value),
    ):
        hold = hold_rate * first + second
        gained.append((w - learn_rate * hold) * norm_gain[:, None])
    totals = lax.psum(tuple(jnp.sum(jnp.abs(g), axis=0) for g in gained), "fsdp")
    factors = tuple(t / rows for t in totals)
    ready = tuple(
        lax.all_gather(
            (g / f).astype(jnp.bfloat16), "fsdp", axis=0, tiled=True
        )
        for g, f in zip(gained, factors)
    )
    return ready + factors


def units_of(cols):
    units = []
    for m, sizes in enumerate(PARTS):
        first = 0
        for size in sizes:
            units.append((m, first, size * cols // UNITS))
            first += size * cols // UNITS
    return units


def diag_slot(units, u):
    m = units[u][0]
    if m < 2:
        return m
    return 2 + sum(unit[0] == 2 for unit in units[:u])


def gather_kernel(total_rows, *refs):
    ins, gain_ref = refs[:9], refs[9]
    outs, factor_ref = refs[10:13], refs[13]
    (
        bufs, gain_line, gain_buf, mine, parts, early,
        load_sem, gain_sem, sum_send, sum_recv, early_send, early_recv,
        x_recv, y_recv, x_rest, y_rest, diag_recv, chip_recv, send_sem,
    ) = refs[14:]
    w_buf, first_buf, second_buf = (bufs.at[k] for k in range(3))
    rows, cols = bufs.shape[2:]
    half = rows // 2

    me = lax.axis_index("fsdp")
    core = me % 2
    x = (me // 2) % 2
    y = me // 4
    partner = me + 1 - 2 * core
    x_near = me + 2 - 4 * x
    y_near = me + 4 - 8 * y
    diag = x_near + 4 - 8 * y
    peers = [
        partner, x_near, y_near, diag,
        x_near + 1 - 2 * core, y_near + 1 - 2 * core, diag + 1 - 2 * core,
    ]
    units = units_of(cols)
    count = len(units)
    early_width = units[0][2]

    barrier = pltpu.get_barrier_semaphore()
    for peer in peers:
        pl.semaphore_signal(
            barrier, inc=1, device_id={"fsdp": peer}, device_id_type=MESH
        )

    def load(u):
        if u < count:
            m, c, width = units[u]
            at = pl.ds(c, width)
            for k in range(3):
                pltpu.make_async_copy(
                    ins[3 * m + k].at[:, at], bufs.at[k, m, :, at],
                    load_sem.at[u % 4],
                ).start()

    def loaded(u):
        m, c, width = units[u]
        ref = bufs.at[:, m, :, pl.ds(c, width)]
        pltpu.make_async_copy(ref, ref, load_sem.at[u % 4]).wait()

    gain_copy = pltpu.make_async_copy(gain_ref, gain_line, gain_sem)
    gain_copy.start()
    for u in range(START):
        load(u)

    gain_copy.wait()
    for k in range(rows // 128):
        line = gain_line[:, pl.ds(k * 128, 128)]
        gain_buf[pl.ds(k * 128, 128), :] = jnp.broadcast_to(line, (128, 128)).T

    def sums(u):
        m, c, width = units[u]
        loaded(u)
        if u == 0:
            for v in range(START, AHEAD):
                load(v)
        load(u + AHEAD)
        tiles = width // 128

        def body(i, acc):
            at = pl.ds(pl.multiple_of(i * STEP, STEP), STEP)
            gain = gain_buf[at, :]
            new = []
            for t in range(tiles):
                lanes = pl.ds(c + t * 128, 128)
                hold = hold_rate * first_buf[m, at, lanes] + second_buf[m, at, lanes]
                gained = (w_buf[m, at, lanes] - learn_rate * hold) * gain
                w_buf[m, at, lanes] = gained
                size = jnp.abs(gained)
                new.append(
                    acc[t] + jnp.sum(size.reshape(STEP // 8, 8, 128), axis=0)
                )
            return tuple(new)

        acc = lax.fori_loop(
            0, rows // STEP, body,
            tuple(jnp.zeros((8, 128), jnp.float32) for _ in range(tiles)),
        )
        for t in range(tiles):
            mine[m, :, pl.ds(c + t * 128, 128)] = jnp.sum(
                acc[t], axis=0, keepdims=True
            )

    def send_sums(u):
        m, c, width = units[u]
        at = pl.ds(c, width)
        for slot, peer in enumerate(peers):
            pltpu.make_async_remote_copy(
                src_ref=mine.at[m, :, at], dst_ref=parts.at[slot, m, :, at],
                send_sem=sum_send, recv_sem=sum_recv.at[u],
                device_id={"fsdp": peer}, device_id_type=MESH,
            ).start()

    def block(m, owner, first, tall, c, width):
        at = pl.ds(pl.multiple_of(owner * rows + first, 16), tall)
        return outs[m].at[at, pl.ds(c, width)]

    def send(m, ref, recv_sem, peer):
        pltpu.make_async_remote_copy(
            src_ref=ref, dst_ref=ref, send_sem=send_sem.at[m], recv_sem=recv_sem,
            device_id={"fsdp": peer}, device_id_type=MESH,
        ).start()

    def arrived(ref, recv_sem):
        pltpu.make_async_remote_copy(
            src_ref=ref, dst_ref=ref, send_sem=send_sem.at[0], recv_sem=recv_sem,
            device_id={"fsdp": partner}, device_id_type=MESH,
        ).wait_recv()

    def early_copy(side, peer):
        return pltpu.make_async_remote_copy(
            src_ref=w_buf.at[0, pl.ds(0, half), pl.ds(0, early_width)],
            dst_ref=early.at[side], send_sem=early_send,
            recv_sem=early_recv.at[side],
            device_id={"fsdp": peer}, device_id_type=MESH,
        )

    def scaled(source, m, owner, lo, hi, c, width):
        scale = jnp.broadcast_to(
            1.0 / factor_ref[pl.ds(m, 1), pl.ds(c, width)], (16, width)
        )

        def body(i, carry):
            for k in range(STEP // 16):
                at = pl.multiple_of(i * STEP + k * 16, 16)
                tile = source[pl.ds(at, 16), pl.ds(c, width)] * scale
                outs[m][
                    pl.ds(pl.multiple_of(owner * rows + at, 16), 16),
                    pl.ds(c, width),
                ] = tile.astype(jnp.bfloat16)
            return carry

        lax.fori_loop(lo // STEP, hi // STEP, body, 0)

    def finish(u):
        m, c, width = units[u]
        at = pl.ds(c, width)
        arrived(parts.at[:, m, :, at], sum_recv.at[u])
        total = mine[m, :, at]
        for slot in range(7):
            total = total + parts[slot, m, :, at]
        factor_ref[pl.ds(m, 1), at] = total / total_rows
        for h in (1, 0):
            scaled(w_buf.at[m], m, me, h * half, (h + 1) * half, c, width)
            if u == 0 and h == 0:
                continue
            ref = block(m, me, h * half, half, c, width)
            send(m, ref, x_recv.at[u] if h == 0 else x_rest.at[m], x_near)
            send(m, ref, y_recv.at[u] if h == 1 else y_rest.at[m], y_near)
        send(m, block(m, me, 0, rows, c, width), chip_recv.at[m], partner)

    def take_early():
        for side, owner in enumerate((x_near, y_near)):
            arrived(early.at[side], early_recv.at[side])
            scaled(early.at[side], 0, owner, 0, half, 0, early_width)

    sums(0)
    pl.semaphore_wait(barrier, 7)
    send_sums(0)
    sums(1)
    send_sums(1)
    early_copy(0, x_near).start()
    early_copy(1, y_near).start()
    for u in range(2, count + 2):
        if u < count:
            sums(u)
            send_sums(u)
        finish(u - 2)
        if u == 3:
            take_early()

    for u, (m, c, width) in enumerate(units):
        ref = block(m, x_near, 0, half, c, width)
        if u > 0:
            arrived(ref, x_recv.at[u])
        send(m, ref, diag_recv.at[0, diag_slot(units, u)], y_near)
        send(m, ref, chip_recv.at[m], partner)
        ref = block(m, y_near, half, half, c, width)
        arrived(ref, y_recv.at[u])
        send(m, ref, diag_recv.at[1, diag_slot(units, u)], x_near)
        send(m, ref, chip_recv.at[m], partner)
        if c + width == cols:
            ref = block(m, x_near, half, half, 0, cols)
            arrived(ref, x_rest.at[m])
            send(m, ref, chip_recv.at[m], partner)
            skip = early_width if m == 0 else 0
            arrived(
                block(m, y_near, 0, half, skip, cols - skip), y_rest.at[m]
            )
            ref = block(m, y_near, 0, half, 0, cols)
            send(m, ref, chip_recv.at[m], partner)
    for u, (m, c, width) in enumerate(units):
        if m < 2:
            if c + width < cols:
                continue
            c, width = 0, cols
        for h in range(2):
            ref = block(m, diag, h * half, half, c, width)
            arrived(ref, diag_recv.at[h, diag_slot(units, u)])
            send(m, ref, chip_recv.at[m], partner)

    for m in range(3):
        taken = outs[m].at[pl.ds(0, 4 * rows), :]
        early_rows = rows * early_width // cols if m == 0 else 0
        sent = outs[m].at[pl.ds(0, 7 * rows - early_rows), :]
        arrived(taken, chip_recv.at[m])
        pltpu.make_async_remote_copy(
            src_ref=sent, dst_ref=sent, send_sem=send_sem.at[m],
            recv_sem=chip_recv.at[m], device_id={"fsdp": partner},
            device_id_type=MESH,
        ).wait_send()
    for ref, sem in ((parts, sum_send), (early, early_send)):
        pltpu.make_async_remote_copy(
            src_ref=ref, dst_ref=ref, send_sem=sem, recv_sem=sum_recv.at[0],
            device_id={"fsdp": partner}, device_id_type=MESH,
        ).wait_send()


def write_kernel(a, b, c, factor, out_a, out_b, out_c, fa, fb, fc, sem):
    copies = []
    for k, (src, dst) in enumerate(((a, out_a), (b, out_b), (c, out_c))):
        rows = src.shape[0] // 4
        for p in range(4):
            at = pl.ds(p * rows, rows)
            copies.append(
                pltpu.make_async_copy(src.at[at, :], dst.at[at, :], sem.at[k, p])
            )
    for copy in copies:
        copy.start()
    for m, out in enumerate((fa, fb, fc)):
        out[...] = factor[m, :]
    for copy in copies:
        copy.wait()


def ringed(*args, total_rows):
    rows, cols = args[0].shape
    units = units_of(cols)
    count = len(units)
    slots = diag_slot(units, count - 1) + 1
    big = (8 * rows, cols)
    vmem = pl.BlockSpec(memory_space=pltpu.VMEM)
    hbm = pl.BlockSpec(memory_space=pltpu.HBM)
    dma = pltpu.SemaphoreType.DMA
    *gathered, factor = pl.pallas_call(
        functools.partial(gather_kernel, total_rows),
        out_shape=[pltpu.VMEM(big, jnp.bfloat16)] * 3
        + [pltpu.VMEM((3, cols), jnp.float32)],
        in_specs=[hbm] * 10,
        out_specs=[vmem] * 4,
        scratch_shapes=[
            pltpu.VMEM((3, 3, rows, cols), jnp.float32),
            pltpu.VMEM((1, rows), jnp.float32),
            pltpu.VMEM((rows, 128), jnp.float32),
            pltpu.VMEM((3, 1, cols), jnp.float32),
            pltpu.VMEM((7, 3, 1, cols), jnp.float32),
            pltpu.VMEM((2, rows // 2, units[0][2]), jnp.float32),
            dma((4,)), dma, dma, dma((count,)), dma, dma((2,)),
            dma((count,)), dma((count,)), dma((3,)), dma((3,)),
            dma((2, slots)), dma((3,)), dma((3,)),
        ],
        compiler_params=pltpu.CompilerParams(
            collective_id=0, has_side_effects=True,
            vmem_limit_bytes=VMEM_BYTES - 3 * 16 * rows * cols - 2**20,
        ),
        name="gather",
    )(*(
        pltpu.with_memory_space_constraint(a, pltpu.HBM)
        for a in (*args[:9], args[9].reshape(1, rows))
    ))
    ready = jax.ShapeDtypeStruct(big, jnp.bfloat16)
    line = jax.ShapeDtypeStruct((cols,), jnp.float32)
    return pl.pallas_call(
        write_kernel,
        out_shape=[ready] * 3 + [line] * 3,
        in_specs=[vmem] * 4,
        out_specs=[hbm] * 3 + [vmem] * 3,
        scratch_shapes=[dma((3, 4))],
        compiler_params=pltpu.CompilerParams(vmem_limit_bytes=2**20),
        name="write",
    )(*gathered, factor)


def on_device(*args, devices):
    rows, cols = args[0].shape
    total_rows = devices * rows
    fits = rows * cols * (36 + 48) <= 48 * 2**20
    if devices == 8 and rows % 128 == 0 and cols % (128 * UNITS) == 0 and fits:
        return tuple(ringed(*args, total_rows=total_rows))
    return plain(*args, rows=total_rows)


def solution(mesh):
    return jax.shard_map(
        functools.partial(on_device, devices=mesh.shape["fsdp"]),
        mesh=mesh,
        in_specs=(P("fsdp", "model"),) * 9 + (P("fsdp"),),
        out_specs=(P(None, "model"),) * 3 + (P("model"),) * 3,
        check_vma=False,
    )
```

```python
import functools
import math

import jax
import jax.numpy as jnp
from jax import lax
from jax.experimental import pallas as pl
from jax.experimental.pallas import tpu as pltpu
from jax.sharding import PartitionSpec as P

learn_rate = 0.2
hold_rate = 0.9
MESH = pl.DeviceIdType.MESH
UNITS = 8
PARTS = ((1, 2, 5), (8,), (8,))
RUNS = (4, 2, 1, 1)
STEP = 32
START = 2
AHEAD = 3
PIECES = 32
VMEM_BYTES = 67_043_328


def plain(
    w_query,
    first_query,
    second_query,
    w_key,
    first_key,
    second_key,
    w_value,
    first_value,
    second_value,
    norm_gain,
    rows,
):
    gained = []
    for w, first, second in (
        (w_query, first_query, second_query),
        (w_key, first_key, second_key),
        (w_value, first_value, second_value),
    ):
        hold = hold_rate * first + second
        gained.append((w - learn_rate * hold) * norm_gain[:, None])
    totals = lax.psum(tuple(jnp.sum(jnp.abs(g), axis=0) for g in gained), "fsdp")
    factors = tuple(t / rows for t in totals)
    ready = tuple(
        lax.all_gather(
            (g / f).astype(jnp.bfloat16), "fsdp", axis=0, tiled=True
        )
        for g, f in zip(gained, factors)
    )
    return ready + factors


def units_of(cols):
    units = []
    for m, sizes in enumerate(PARTS):
        first = 0
        for size in sizes:
            units.append((m, first, size * cols // UNITS))
            first += size * cols // UNITS
    return units


def runs_of(cols):
    runs = []
    first = 0
    for size in RUNS:
        runs.append((first, size * cols // UNITS))
        first += size * cols // UNITS
    return runs


def gather_kernel(total_rows, *refs):
    ins, gain_ref = refs[:9], refs[9]
    outs, factors = refs[10], refs[11:14]
    (
        bufs, gain_line, gain_buf, mine, parts, early,
        load_sem, gain_sem, sum_send, sum_recv, early_send, early_recv,
        x_recv, y_recv, x_rest, y_rest, diag_recv, hand_recv, more_recv,
        chip_recv, send_sem,
    ) = refs[14:]
    w_buf, first_buf, second_buf = (bufs.at[k] for k in range(3))
    rows, cols = bufs.shape[2:]
    half = rows // 2

    me = lax.axis_index("fsdp")
    core = me % 2
    x = (me // 2) % 2
    y = me // 4
    partner = me + 1 - 2 * core
    x_near = me + 2 - 4 * x
    y_near = me + 4 - 8 * y
    diag = x_near + 4 - 8 * y
    peers = [
        partner, x_near, y_near, diag,
        x_near + 1 - 2 * core, y_near + 1 - 2 * core, diag + 1 - 2 * core,
    ]
    units = units_of(cols)
    runs = runs_of(cols)
    count = len(units)
    early_width = units[0][2]
    early_rows = half * early_width // cols
    last_first, last_width = runs[-1]
    last_rows = rows * last_width // cols

    barrier = pltpu.get_barrier_semaphore()
    for peer in peers:
        pl.semaphore_signal(
            barrier, inc=1, device_id={"fsdp": peer}, device_id_type=MESH
        )

    def load(u):
        if u < count:
            m, c, width = units[u]
            at = pl.ds(c, width)
            for k in range(3):
                pltpu.make_async_copy(
                    ins[3 * m + k].at[:, at], bufs.at[k, m, :, at],
                    load_sem.at[u % 4],
                ).start()

    def loaded(u):
        m, c, width = units[u]
        ref = bufs.at[:, m, :, pl.ds(c, width)]
        pltpu.make_async_copy(ref, ref, load_sem.at[u % 4]).wait()

    gain_copy = pltpu.make_async_copy(gain_ref, gain_line, gain_sem)
    gain_copy.start()
    for u in range(START):
        load(u)

    gain_copy.wait()
    for k in range(rows // 128):
        line = gain_line[:, pl.ds(k * 128, 128)]
        gain_buf[pl.ds(k * 128, 128), :] = jnp.broadcast_to(line, (128, 128)).T

    def sums(u):
        m, c, width = units[u]
        loaded(u)
        if u == 0:
            for v in range(START, AHEAD):
                load(v)
        load(u + AHEAD)
        tiles = width // 128

        def body(i, acc):
            at = pl.ds(pl.multiple_of(i * STEP, STEP), STEP)
            gain = gain_buf[at, :]
            new = []
            for t in range(tiles):
                lanes = pl.ds(c + t * 128, 128)
                hold = hold_rate * first_buf[m, at, lanes] + second_buf[m, at, lanes]
                gained = (w_buf[m, at, lanes] - learn_rate * hold) * gain
                w_buf[m, at, lanes] = gained
                size = jnp.abs(gained)
                new.append(
                    acc[t] + jnp.sum(size.reshape(STEP // 8, 8, 128), axis=0)
                )
            return tuple(new)

        acc = lax.fori_loop(
            0, rows // STEP, body,
            tuple(jnp.zeros((8, 128), jnp.float32) for _ in range(tiles)),
        )
        for t in range(tiles):
            mine[m, :, pl.ds(c + t * 128, 128)] = jnp.sum(
                acc[t], axis=0, keepdims=True
            )

    def send_sums(u):
        m, c, width = units[u]
        at = pl.ds(c, width)
        for slot, peer in enumerate(peers):
            pltpu.make_async_remote_copy(
                src_ref=mine.at[m, :, at], dst_ref=parts.at[slot, m, :, at],
                send_sem=sum_send, recv_sem=sum_recv.at[u],
                device_id={"fsdp": peer}, device_id_type=MESH,
            ).start()

    def block(m, owner, first, tall, c, width):
        at = pl.multiple_of((8 * m + owner) * rows + first, 16)
        return outs.at[pl.ds(at, tall), pl.ds(c, width)]

    def span(tall):
        return outs.at[pl.ds(0, tall), :]

    def send(ref, recv_sem, peer):
        pltpu.make_async_remote_copy(
            src_ref=ref, dst_ref=ref, send_sem=send_sem, recv_sem=recv_sem,
            device_id={"fsdp": peer}, device_id_type=MESH,
        ).start()

    def arrived(ref, recv_sem):
        pltpu.make_async_remote_copy(
            src_ref=ref, dst_ref=ref, send_sem=send_sem, recv_sem=recv_sem,
            device_id={"fsdp": partner}, device_id_type=MESH,
        ).wait_recv()

    def left(ref, sem):
        pltpu.make_async_remote_copy(
            src_ref=ref, dst_ref=ref, send_sem=sem, recv_sem=chip_recv,
            device_id={"fsdp": partner}, device_id_type=MESH,
        ).wait_send()

    def early_copy(side, peer):
        return pltpu.make_async_remote_copy(
            src_ref=w_buf.at[0, pl.ds(0, half), pl.ds(0, early_width)],
            dst_ref=early.at[side], send_sem=early_send,
            recv_sem=early_recv.at[side],
            device_id={"fsdp": peer}, device_id_type=MESH,
        )

    def scaled(source, m, owner, lo, hi, c, width):
        scale = jnp.broadcast_to(
            1.0 / factors[m][:, pl.ds(c, width)], (16, width)
        )

        def body(i, carry):
            for k in range(STEP // 16):
                at = pl.multiple_of(i * STEP + k * 16, 16)
                tile = source[pl.ds(at, 16), pl.ds(c, width)] * scale
                outs[
                    pl.ds(pl.multiple_of((8 * m + owner) * rows + at, 16), 16),
                    pl.ds(c, width),
                ] = tile.astype(jnp.bfloat16)
            return carry

        lax.fori_loop(lo // STEP, hi // STEP, body, 0)

    def finish(u):
        m, c, width = units[u]
        at = pl.ds(c, width)
        arrived(parts.at[:, m, :, at], sum_recv.at[u])
        total = mine[m, :, at]
        for slot in range(7):
            total = total + parts[slot, m, :, at]
        factors[m][:, at] = total / total_rows
        for h in (1, 0):
            scaled(w_buf.at[m], m, me, h * half, (h + 1) * half, c, width)
            if u == 0 and h == 0:
                continue
            ref = block(m, me, h * half, half, c, width)
            near, rest = (x_near, y_near) if h == 0 else (y_near, x_near)
            recv, rest_recv = (x_recv, y_rest) if h == 0 else (y_recv, x_rest)
            send(ref, rest_recv, rest)
            if m < 2:
                send(ref, recv.at[0], near)
            else:
                for r, (first, wide) in enumerate(runs):
                    send(
                        block(m, me, h * half, half, first, wide),
                        recv.at[1 + r], near,
                    )
        send(block(m, me, 0, rows, c, width), chip_recv, partner)

    def take_early():
        for side, owner in enumerate((x_near, y_near)):
            arrived(early.at[side], early_recv.at[side])
            scaled(early.at[side], 0, owner, 0, half, 0, early_width)

    def pass_on(ref, slot, h, near):
        send(ref, diag_recv.at[h, slot], near)
        send(ref, chip_recv, partner)

    sums(0)
    pl.semaphore_wait(barrier, 7)
    send_sums(0)
    sums(1)
    send_sums(1)
    early_copy(0, x_near).start()
    early_copy(1, y_near).start()
    sums(2)
    send_sums(2)
    finish(0)
    finish(1)
    take_early()
    for u in range(3, count):
        sums(u)
        send_sums(u)
        finish(u - 1)
    finish(count - 1)

    arrived(span(2 * half - early_rows), x_recv.at[0])
    arrived(span(2 * half), y_recv.at[0])
    for m in range(2):
        pass_on(block(m, x_near, 0, half, 0, cols), 0, 0, y_near)
        pass_on(block(m, y_near, half, half, 0, cols), 0, 1, x_near)
    for r, (c, width) in enumerate(runs[:-1]):
        ref = block(2, x_near, 0, half, c, width)
        arrived(ref, x_recv.at[1 + r])
        pass_on(ref, 1 + r, 0, y_near)
        ref = block(2, y_near, half, half, c, width)
        arrived(ref, y_recv.at[1 + r])
        pass_on(ref, 1 + r, 1, x_near)

    slot = len(runs)
    x_last = block(2, x_near, 0, half, last_first, last_width)
    y_last = block(2, y_near, half, half, last_first, last_width)
    arrived(x_last, x_recv.at[slot])
    arrived(y_last, y_recv.at[slot])

    @pl.when(core == 0)
    def _():
        send(x_last, hand_recv.at[0], partner)
        send(y_last, hand_recv.at[1], partner)

    @pl.when(core == 1)
    def _():
        pass_on(x_last, slot, 0, y_near)
        pass_on(y_last, slot, 1, x_near)
        ref = block(2, x_near - 1, 0, half, last_first, last_width)
        arrived(ref, hand_recv.at[0])
        send(ref, more_recv.at[0], y_near)
        ref = block(2, y_near - 1, half, half, last_first, last_width)
        arrived(ref, hand_recv.at[1])
        send(ref, more_recv.at[1], x_near)

    arrived(span(3 * half), x_rest)
    arrived(span(3 * half - early_rows), y_rest)
    for m in range(3):
        send(block(m, x_near, half, half, 0, cols), chip_recv, partner)
        send(block(m, y_near, 0, half, 0, cols), chip_recv, partner)

    for h in range(2):
        arrived(span(2 * half), diag_recv.at[h, 0])
        for m in range(2):
            send(block(m, diag, h * half, half, 0, cols), chip_recv, partner)
    for r, (c, width) in enumerate(runs[:-1]):
        for h in range(2):
            ref = block(2, diag, h * half, half, c, width)
            arrived(ref, diag_recv.at[h, 1 + r])
            send(ref, chip_recv, partner)

    @pl.when(core == 0)
    def _():
        arrived(span(12 * rows + last_rows), chip_recv)
        left(span(21 * rows - 2 * early_rows - 2 * last_rows), send_sem)

    @pl.when(core == 1)
    def _():
        for owner, recv in ((diag, diag_recv.at[:, slot]), (diag - 1, more_recv)):
            for h in range(2):
                ref = block(2, owner, h * half, half, last_first, last_width)
                arrived(ref, recv.at[h])
                send(ref, chip_recv, partner)
        arrived(span(12 * rows - 2 * last_rows), chip_recv)
        left(span(21 * rows - 2 * early_rows + 2 * last_rows), send_sem)

    left(parts, sum_send)
    left(early, early_send)


def write_kernel(*refs):
    src, outs, sem = refs[0], refs[4:7], refs[10]
    lines = [
        pltpu.make_async_copy(refs[1 + k], refs[7 + k], sem.at[3 + k])
        for k in range(3)
    ]
    for line in lines:
        line.start()
    tall = outs[0].shape[0]
    step = tall // PIECES
    for k in range(3):
        for p in range(PIECES):
            pltpu.make_async_copy(
                src.at[pl.ds(k * tall + p * step, step), :],
                outs[k].at[pl.ds(p * step, step), :], sem.at[k],
            ).start()
    for k in range(3):
        whole = src.at[pl.ds(k * tall, tall), :]
        pltpu.make_async_copy(whole, outs[k], sem.at[k]).wait()
    for line in lines:
        line.wait()


def ringed(*args, total_rows):
    rows, cols = args[0].shape
    units = units_of(cols)
    count = len(units)
    slots = len(RUNS) + 1
    big = (8 * rows, cols)
    vmem = pl.BlockSpec(memory_space=pltpu.VMEM)
    hbm = pl.BlockSpec(memory_space=pltpu.HBM)
    dma = pltpu.SemaphoreType.DMA
    gathered = pl.pallas_call(
        functools.partial(gather_kernel, total_rows),
        out_shape=[pltpu.VMEM((24 * rows, cols), jnp.bfloat16)]
        + [pltpu.VMEM((1, cols), jnp.float32)] * 3,
        in_specs=[hbm] * 10,
        out_specs=[vmem] * 4,
        scratch_shapes=[
            pltpu.VMEM((3, 3, rows, cols), jnp.float32),
            pltpu.VMEM((1, rows), jnp.float32),
            pltpu.VMEM((rows, 128), jnp.float32),
            pltpu.VMEM((3, 1, cols), jnp.float32),
            pltpu.VMEM((7, 3, 1, cols), jnp.float32),
            pltpu.VMEM((2, rows // 2, units[0][2]), jnp.float32),
            dma((4,)), dma, dma, dma((count,)), dma, dma((2,)),
            dma((slots,)), dma((slots,)), dma, dma,
            dma((2, slots)), dma((2,)), dma((2,)), dma, dma,
        ],
        compiler_params=pltpu.CompilerParams(
            collective_id=0, has_side_effects=True,
            vmem_limit_bytes=VMEM_BYTES - 3 * 16 * rows * cols - 2**20,
        ),
        name="gather",
    )(*(
        pltpu.with_memory_space_constraint(a, pltpu.HBM)
        for a in (*args[:9], args[9].reshape(1, rows))
    ))
    ready = jax.ShapeDtypeStruct(big, jnp.bfloat16)
    line = jax.ShapeDtypeStruct((1, cols), jnp.float32)
    *ready, a, b, c = pl.pallas_call(
        write_kernel,
        out_shape=[ready] * 3 + [line] * 3,
        in_specs=[vmem] * 4,
        out_specs=[hbm] * 6,
        scratch_shapes=[dma((6,))],
        compiler_params=pltpu.CompilerParams(vmem_limit_bytes=2**20),
        name="write",
    )(*gathered)
    return ready + [f.reshape(cols) for f in (a, b, c)]


def on_device(*args, devices):
    rows, cols = args[0].shape
    total_rows = devices * rows
    fits = rows * cols * (36 + 48) <= 48 * 2**20
    if devices == 8 and rows % 128 == 0 and cols % (128 * UNITS) == 0 and fits:
        return tuple(ringed(*args, total_rows=total_rows))
    return plain(*args, rows=total_rows)


def solution(mesh):
    return jax.shard_map(
        functools.partial(on_device, devices=mesh.shape["fsdp"]),
        mesh=mesh,
        in_specs=(P("fsdp", "model"),) * 9 + (P("fsdp"),),
        out_specs=(P(None, "model"),) * 3 + (P("model"),) * 3,
        check_vma=False,
    )
```

```python
import functools
import math

import jax
import jax.numpy as jnp
from jax import lax
from jax.experimental import pallas as pl
from jax.experimental.pallas import tpu as pltpu
from jax.sharding import PartitionSpec as P

learn_rate = 0.2
hold_rate = 0.9
MESH = pl.DeviceIdType.MESH
UNITS = 8
PARTS = ((1, 2, 5), (8,), (8,))
KEY_RUNS = (4, 2, 2)
VALUE_RUNS = (2, 2, 2, 1, 1)
STEP = 32
START = 2
AHEAD = 3
PIECES = 32
VMEM_BYTES = 67_043_328


def plain(
    w_query,
    first_query,
    second_query,
    w_key,
    first_key,
    second_key,
    w_value,
    first_value,
    second_value,
    norm_gain,
    rows,
):
    gained = []
    for w, first, second in (
        (w_query, first_query, second_query),
        (w_key, first_key, second_key),
        (w_value, first_value, second_value),
    ):
        hold = hold_rate * first + second
        gained.append((w - learn_rate * hold) * norm_gain[:, None])
    totals = lax.psum(tuple(jnp.sum(jnp.abs(g), axis=0) for g in gained), "fsdp")
    factors = tuple(t / rows for t in totals)
    ready = tuple(
        lax.all_gather(
            (g / f).astype(jnp.bfloat16), "fsdp", axis=0, tiled=True
        )
        for g, f in zip(gained, factors)
    )
    return ready + factors


def units_of(cols):
    units = []
    for m, sizes in enumerate(PARTS):
        first = 0
        for size in sizes:
            units.append((m, first, size * cols // UNITS))
            first += size * cols // UNITS
    return units


def runs_of(sizes, cols):
    runs = []
    first = 0
    for size in sizes:
        runs.append((first, size * cols // UNITS))
        first += size * cols // UNITS
    return runs


def places():
    me = lax.axis_index("fsdp")
    core = me % 2
    x = (me // 2) % 2
    y = me // 4
    partner = me + 1 - 2 * core
    x_near = me + 2 - 4 * x
    y_near = me + 4 - 8 * y
    diag = x_near + 4 - 8 * y
    return me, core, partner, x_near, y_near, diag


def gather_kernel(total_rows, *refs):
    ins, gain_ref = refs[:9], refs[9]
    outs, value, factors = refs[10], refs[11], refs[12:15]
    (
        bufs, gain_line, gain_buf, mine, parts, early,
        load_sem, gain_sem, sum_send, sum_recv, early_send, early_recv,
        x_recv, y_recv, x_rest, y_rest, diag_recv, x_value, y_value,
        chip_recv, chip_value, send_sem,
    ) = refs[15:]
    w_buf, first_buf, second_buf = (bufs.at[k] for k in range(3))
    rows, cols = bufs.shape[2:]
    half = rows // 2

    me, core, partner, x_near, y_near, diag = places()
    peers = [
        diag + 1 - 2 * core, diag, x_near + 1 - 2 * core, y_near + 1 - 2 * core,
        x_near, y_near, partner,
    ]
    units = units_of(cols)
    runs = runs_of(KEY_RUNS, cols)
    count = len(units)
    early_width = units[0][2]
    early_rows = half * early_width // cols

    barrier = pltpu.get_barrier_semaphore()
    for peer in peers:
        pl.semaphore_signal(
            barrier, inc=1, device_id={"fsdp": peer}, device_id_type=MESH
        )

    def load(u):
        if u < count:
            m, c, width = units[u]
            at = pl.ds(c, width)
            for k in range(3):
                pltpu.make_async_copy(
                    ins[3 * m + k].at[:, at], bufs.at[k, m, :, at],
                    load_sem.at[u % 4],
                ).start()

    def loaded(u):
        m, c, width = units[u]
        ref = bufs.at[:, m, :, pl.ds(c, width)]
        pltpu.make_async_copy(ref, ref, load_sem.at[u % 4]).wait()

    gain_copy = pltpu.make_async_copy(gain_ref, gain_line, gain_sem)
    gain_copy.start()
    for u in range(START):
        load(u)

    gain_copy.wait()
    for k in range(rows // 128):
        line = gain_line[:, pl.ds(k * 128, 128)]
        gain_buf[pl.ds(k * 128, 128), :] = jnp.broadcast_to(line, (128, 128)).T

    def sums(u):
        m, c, width = units[u]
        loaded(u)
        if u == 0:
            for v in range(START, AHEAD):
                load(v)
        load(u + AHEAD)
        tiles = width // 128

        def body(i, acc):
            at = pl.ds(pl.multiple_of(i * STEP, STEP), STEP)
            gain = gain_buf[at, :]
            new = []
            for t in range(tiles):
                lanes = pl.ds(c + t * 128, 128)
                hold = hold_rate * first_buf[m, at, lanes] + second_buf[m, at, lanes]
                gained = (w_buf[m, at, lanes] - learn_rate * hold) * gain
                w_buf[m, at, lanes] = gained
                size = jnp.abs(gained)
                new.append(
                    acc[t] + jnp.sum(size.reshape(STEP // 8, 8, 128), axis=0)
                )
            return tuple(new)

        acc = lax.fori_loop(
            0, rows // STEP, body,
            tuple(jnp.zeros((8, 128), jnp.float32) for _ in range(tiles)),
        )
        for t in range(tiles):
            mine[m, :, pl.ds(c + t * 128, 128)] = jnp.sum(
                acc[t], axis=0, keepdims=True
            )

    def send_sums(u):
        m, c, width = units[u]
        at = pl.ds(c, width)
        for slot, peer in enumerate(peers):
            pltpu.make_async_remote_copy(
                src_ref=mine.at[m, :, at], dst_ref=parts.at[slot, m, :, at],
                send_sem=sum_send, recv_sem=sum_recv.at[u],
                device_id={"fsdp": peer}, device_id_type=MESH,
            ).start()

    def block(m, owner, first, tall, c, width):
        ref = value if m == 2 else outs
        at = owner * rows + first
        if m == 1:
            at = at + 8 * rows
        at = pl.multiple_of(at, 16)
        return ref.at[pl.ds(at, tall), pl.ds(c, width)]

    def span(tall):
        return outs.at[pl.ds(0, tall), :]

    def send(ref, recv_sem, peer):
        pltpu.make_async_remote_copy(
            src_ref=ref, dst_ref=ref, send_sem=send_sem, recv_sem=recv_sem,
            device_id={"fsdp": peer}, device_id_type=MESH,
        ).start()

    def arrived(ref, recv_sem):
        pltpu.make_async_remote_copy(
            src_ref=ref, dst_ref=ref, send_sem=send_sem, recv_sem=recv_sem,
            device_id={"fsdp": partner}, device_id_type=MESH,
        ).wait_recv()

    def left(ref, sem):
        pltpu.make_async_remote_copy(
            src_ref=ref, dst_ref=ref, send_sem=sem, recv_sem=chip_recv,
            device_id={"fsdp": partner}, device_id_type=MESH,
        ).wait_send()

    def early_copy(side, peer):
        return pltpu.make_async_remote_copy(
            src_ref=w_buf.at[0, pl.ds(0, half), pl.ds(0, early_width)],
            dst_ref=early.at[side], send_sem=early_send,
            recv_sem=early_recv.at[side],
            device_id={"fsdp": peer}, device_id_type=MESH,
        )

    def scaled(source, m, owner, lo, hi, c, width):
        scale = jnp.broadcast_to(
            1.0 / factors[m][:, pl.ds(c, width)], (16, width)
        )

        def body(i, carry):
            for k in range(STEP // 16):
                at = pl.multiple_of(i * STEP + k * 16, 16)
                tile = source[pl.ds(at, 16), pl.ds(c, width)] * scale
                block(m, owner, at, 16, c, width)[...] = tile.astype(jnp.bfloat16)
            return carry

        lax.fori_loop(lo // STEP, hi // STEP, body, 0)

    def finish(u):
        m, c, width = units[u]
        at = pl.ds(c, width)
        arrived(parts.at[:, m, :, at], sum_recv.at[u])
        total = mine[m, :, at]
        for slot in range(7):
            total = total + parts[slot, m, :, at]
        factors[m][:, at] = total / total_rows
        for h in (1, 0):
            scaled(w_buf.at[m], m, me, h * half, (h + 1) * half, c, width)
            if m == 2 or u == 0 and h == 0:
                continue
            ref = block(m, me, h * half, half, c, width)
            send(ref, x_recv.at[m] if h == 0 else x_rest, x_near)
            send(ref, y_recv.at[m] if h == 1 else y_rest, y_near)
        send(
            block(m, me, 0, rows, c, width),
            chip_value if m == 2 else chip_recv, partner,
        )

    def take_early():
        for side, owner in enumerate((x_near, y_near)):
            arrived(early.at[side], early_recv.at[side])
            scaled(early.at[side], 0, owner, 0, half, 0, early_width)

    sums(0)
    pl.semaphore_wait(barrier, 7)
    send_sums(0)
    sums(1)
    send_sums(1)
    early_copy(0, x_near).start()
    early_copy(1, y_near).start()
    sums(2)
    send_sums(2)
    finish(0)
    finish(1)
    take_early()
    for u in range(3, count):
        sums(u)
        send_sums(u)
        finish(u - 1)
    finish(count - 1)

    for m in range(2):
        arrived(span(half - early_rows * (m == 0)), x_recv.at[m])
        arrived(span(half), y_recv.at[m])
        pieces = enumerate(runs) if m == 1 else [(-1, (0, cols))]
        for r, (c, width) in pieces:
            send(
                block(m, x_near, 0, half, c, width), diag_recv.at[0, 1 + r], y_near
            )
            send(
                block(m, y_near, half, half, c, width), diag_recv.at[1, 1 + r],
                x_near,
            )

    mine_value = block(2, me, 0, rows, 0, cols)

    @pl.when(core == 0)
    def _():
        send(mine_value, x_value, x_near)
        send(mine_value, y_value, y_near)

    arrived(span(2 * half), x_rest)
    arrived(span(2 * half - early_rows), y_rest)
    for m in range(2):
        send(block(m, x_near, 0, rows, 0, cols), chip_recv, partner)
        send(block(m, y_near, 0, rows, 0, cols), chip_recv, partner)
    for m in range(2):
        pieces = enumerate(runs) if m == 1 else [(-1, (0, cols))]
        for r, (c, width) in pieces:
            for h in range(2):
                ref = block(m, diag, h * half, half, c, width)
                arrived(ref, diag_recv.at[h, 1 + r])
                send(ref, chip_recv, partner)
    arrived(span(8 * rows), chip_recv)
    arrived(span(rows), chip_value)

    @pl.when(core == 0)
    def _():
        arrived(span(rows), x_value)
        arrived(span(rows), y_value)
        left(span(15 * rows - 2 * early_rows), send_sem)
        left(span(2 * rows), send_sem)

    @pl.when(core == 1)
    def _():
        left(span(15 * rows - 2 * early_rows), send_sem)

    left(parts, sum_send)
    left(early, early_send)


def value_kernel(held, token, value, *sems):
    (
        x_recv, y_recv, x_rest, y_rest, diag_recv, chip_recv, send_sem, ready,
    ) = sems
    cols = held.shape[1]
    rows = held.shape[0] // 8
    half = rows // 2
    me, core, partner, x_near, y_near, diag = places()
    runs = runs_of(VALUE_RUNS, cols)

    barrier = pltpu.get_barrier_semaphore()
    for peer in (x_near, y_near):
        pl.semaphore_signal(
            barrier, inc=1, device_id={"fsdp": peer}, device_id_type=MESH
        )

    @pl.when(core == 1)
    def _():
        pl.semaphore_signal(
            barrier, inc=1, device_id={"fsdp": partner}, device_id_type=MESH
        )

    pl.semaphore_wait(barrier, 3 - core)

    def block(ref, owner, first, tall, c, width):
        at = pl.multiple_of(owner * rows + first, 16)
        return ref.at[pl.ds(at, tall), pl.ds(c, width)]

    def send(source, owner, first, tall, c, width, recv_sem, peer):
        pltpu.make_async_remote_copy(
            src_ref=block(source, owner, first, tall, c, width),
            dst_ref=block(value, owner, first, tall, c, width),
            send_sem=send_sem, recv_sem=recv_sem,
            device_id={"fsdp": peer}, device_id_type=MESH,
        ).start()

    def copy_of(ref, recv_sem):
        return pltpu.make_async_remote_copy(
            src_ref=ref, dst_ref=ref, send_sem=send_sem, recv_sem=recv_sem,
            device_id={"fsdp": partner}, device_id_type=MESH,
        )

    def forward(source, r, c, width):
        send(source, x_near, 0, half, c, width, diag_recv.at[0, r], y_near)
        send(source, y_near, half, half, c, width, diag_recv.at[1, r], x_near)

    def cross(source):
        for owner in (x_near, y_near):
            send(source, owner, 0, rows, 0, cols, chip_recv, partner)

    @pl.when(core == 0)
    def _():
        pl.semaphore_signal(
            ready, inc=1, device_id={"fsdp": partner}, device_id_type=MESH
        )
        for r, (c, width) in enumerate(runs):
            forward(held, r, c, width)
        cross(held)

    @pl.when(core == 1)
    def _():
        for r, (c, width) in enumerate(runs):
            send(held, me, 0, half, c, width, x_recv.at[r], x_near)
            send(held, me, half, half, c, width, y_recv.at[r], y_near)
        send(held, me, half, half, 0, cols, x_rest, x_near)
        send(held, me, 0, half, 0, cols, y_rest, y_near)
        for r, (c, width) in enumerate(runs):
            copy_of(block(value, x_near, 0, half, c, width), x_recv.at[r]).wait_recv()
            copy_of(
                block(value, y_near, half, half, c, width), y_recv.at[r]
            ).wait_recv()
            forward(value, r, c, width)
        copy_of(block(value, x_near, half, half, 0, cols), x_rest).wait_recv()
        copy_of(block(value, y_near, 0, half, 0, cols), y_rest).wait_recv()
        pl.semaphore_wait(ready, 1)
        cross(value)

    for r, (c, width) in enumerate(runs):
        for h in range(2):
            copy_of(
                block(value, diag, h * half, half, c, width), diag_recv.at[h, r]
            ).wait_recv()
            send(value, diag, h * half, half, c, width, chip_recv, partner)
    copy_of(value.at[pl.ds(0, 3 * rows), :], chip_recv).wait_recv()

    @pl.when(core == 0)
    def _():
        copy_of(value.at[pl.ds(0, 4 * rows), :], chip_recv).wait_send()

    @pl.when(core == 1)
    def _():
        copy_of(value.at[pl.ds(0, 6 * rows), :], chip_recv).wait_send()


def write_pair(src, *refs):
    lines, outs, line_outs, sem = refs[:3], refs[3:5], refs[5:8], refs[8]
    copies = [
        pltpu.make_async_copy(lines[k], line_outs[k], sem.at[2 + k])
        for k in range(3)
    ]
    for copy in copies:
        copy.start()
    tall = outs[0].shape[0]
    step = tall // PIECES
    for k in range(2):
        for p in range(PIECES):
            pltpu.make_async_copy(
                src.at[pl.ds(k * tall + p * step, step), :],
                outs[k].at[pl.ds(p * step, step), :], sem.at[k],
            ).start()
    for k in range(2):
        whole = src.at[pl.ds(k * tall, tall), :]
        pltpu.make_async_copy(whole, outs[k], sem.at[k]).wait()
    for copy in copies:
        copy.wait()


def write_value(held, value, out, sem):
    rows = out.shape[0] // 8
    me, core, _, x_near, y_near, diag = places()
    step = 8 * rows // PIECES

    def put(src, first):
        for p in range(rows // step):
            at = pl.ds(pl.multiple_of(first * rows + p * step, 16), step)
            pltpu.make_async_copy(src.at[at, :], out.at[at, :], sem).start()

    for k in range(2):
        put(held, me - core + k)
        put(value, diag - core + k)
    for near in (x_near, y_near):
        put(value, near + 1 - 2 * core)

    @pl.when(core == 0)
    def _():
        put(held, x_near)
        put(held, y_near)

    @pl.when(core == 1)
    def _():
        put(value, x_near)
        put(value, y_near)

    pltpu.make_async_copy(value, out, sem).wait()


def ringed(*args, total_rows):
    rows, cols = args[0].shape
    units = units_of(cols)
    count = len(units)
    vmem = pl.BlockSpec(memory_space=pltpu.VMEM)
    hbm = pl.BlockSpec(memory_space=pltpu.HBM)
    dma = pltpu.SemaphoreType.DMA
    held = pltpu.VMEM((8 * rows, cols), jnp.bfloat16)
    runs = len(VALUE_RUNS)
    slots = len(KEY_RUNS) + 1
    pair, held_value, *factors = pl.pallas_call(
        functools.partial(gather_kernel, total_rows),
        out_shape=[pltpu.VMEM((16 * rows, cols), jnp.bfloat16), held]
        + [pltpu.VMEM((1, cols), jnp.float32)] * 3,
        in_specs=[hbm] * 10,
        out_specs=[vmem] * 5,
        scratch_shapes=[
            pltpu.VMEM((3, 3, rows, cols), jnp.float32),
            pltpu.VMEM((1, rows), jnp.float32),
            pltpu.VMEM((rows, 128), jnp.float32),
            pltpu.VMEM((3, 1, cols), jnp.float32),
            pltpu.VMEM((7, 3, 1, cols), jnp.float32),
            pltpu.VMEM((2, rows // 2, units[0][2]), jnp.float32),
            dma((4,)), dma, dma, dma((count,)), dma, dma((2,)),
            dma((2,)), dma((2,)), dma, dma, dma((2, slots)), dma, dma,
            dma, dma, dma,
        ],
        compiler_params=pltpu.CompilerParams(
            collective_id=0, has_side_effects=True,
            vmem_limit_bytes=VMEM_BYTES - 3 * 16 * rows * cols - 2**20,
        ),
        name="gather",
    )(*(
        pltpu.with_memory_space_constraint(a, pltpu.HBM)
        for a in (*args[:9], args[9].reshape(1, rows))
    ))
    ready = jax.ShapeDtypeStruct((8 * rows, cols), jnp.bfloat16)
    line = jax.ShapeDtypeStruct((1, cols), jnp.float32)
    query, key, *lines = pl.pallas_call(
        write_pair,
        out_shape=[ready] * 2 + [line] * 3,
        in_specs=[vmem] * 4,
        out_specs=[hbm] * 5,
        scratch_shapes=[dma((5,))],
        compiler_params=pltpu.CompilerParams(
            has_side_effects=True, vmem_limit_bytes=2**20
        ),
        name="write_pair",
    )(pair, *factors)
    value = pl.pallas_call(
        value_kernel,
        out_shape=held,
        in_specs=[vmem, hbm],
        out_specs=vmem,
        scratch_shapes=[
            dma((runs,)), dma((runs,)), dma, dma, dma((2, runs)), dma, dma,
            pltpu.SemaphoreType.REGULAR,
        ],
        compiler_params=pltpu.CompilerParams(
            collective_id=1, has_side_effects=True, vmem_limit_bytes=2**20
        ),
        name="value",
    )(held_value, pltpu.with_memory_space_constraint(lines[0], pltpu.HBM))
    value = pl.pallas_call(
        write_value,
        out_shape=ready,
        in_specs=[vmem] * 2,
        out_specs=hbm,
        scratch_shapes=[dma],
        compiler_params=pltpu.CompilerParams(vmem_limit_bytes=2**20),
        name="write_value",
    )(held_value, value)
    return [query, key, value] + [f.reshape(cols) for f in lines]


def on_device(*args, devices):
    rows, cols = args[0].shape
    total_rows = devices * rows
    fits = rows * cols * (36 + 48) <= 48 * 2**20
    if devices == 8 and rows % 128 == 0 and cols % (128 * UNITS) == 0 and fits:
        return tuple(ringed(*args, total_rows=total_rows))
    return plain(*args, rows=total_rows)


def solution(mesh):
    return jax.shard_map(
        functools.partial(on_device, devices=mesh.shape["fsdp"]),
        mesh=mesh,
        in_specs=(P("fsdp", "model"),) * 9 + (P("fsdp"),),
        out_specs=(P(None, "model"),) * 3 + (P("model"),) * 3,
        check_vma=False,
    )
```

```python
import functools
import math

import jax
import jax.numpy as jnp
from jax import lax
from jax.experimental import pallas as pl
from jax.experimental.pallas import tpu as pltpu
from jax.sharding import PartitionSpec as P

learn_rate = 0.2
hold_rate = 0.9
MESH = pl.DeviceIdType.MESH
UNITS = 8
PARTS = ((1, 2, 5), (8,), (2, 6))
HEAD_RUNS = (1, 1)
TAIL_RUNS = (2, 2, 1, 1)
SPLIT = 2
EARLY = 64
STEP = 32
START = 2
AHEAD = 3
PIECES = 32
VMEM_BYTES = 67_043_328


def plain(
    w_query,
    first_query,
    second_query,
    w_key,
    first_key,
    second_key,
    w_value,
    first_value,
    second_value,
    norm_gain,
    rows,
):
    gained = []
    for w, first, second in (
        (w_query, first_query, second_query),
        (w_key, first_key, second_key),
        (w_value, first_value, second_value),
    ):
        hold = hold_rate * first + second
        gained.append((w - learn_rate * hold) * norm_gain[:, None])
    totals = lax.psum(tuple(jnp.sum(jnp.abs(g), axis=0) for g in gained), "fsdp")
    factors = tuple(t / rows for t in totals)
    ready = tuple(
        lax.all_gather(
            (g / f).astype(jnp.bfloat16), "fsdp", axis=0, tiled=True
        )
        for g, f in zip(gained, factors)
    )
    return ready + factors


def units_of(cols):
    units = []
    for m, sizes in enumerate(PARTS):
        first = 0
        for size in sizes:
            units.append((m, first, size * cols // UNITS))
            first += size * cols // UNITS
    return units


def runs_of(sizes, cols, parts):
    runs = []
    first = 0
    for size in sizes:
        runs.append((first, size * cols // parts))
        first += size * cols // parts
    return runs


def places():
    me = lax.axis_index("fsdp")
    core = me % 2
    x = (me // 2) % 2
    y = me // 4
    partner = me + 1 - 2 * core
    x_near = me + 2 - 4 * x
    y_near = me + 4 - 8 * y
    diag = x_near + 4 - 8 * y
    return me, core, partner, x_near, y_near, diag


def block_of(ref, at, tall, c, width):
    return ref.at[pl.ds(pl.multiple_of(at, 16), tall), pl.ds(c, width)]


class Relay:
    def __init__(self, own, far, sems, send_sem):
        self.own, self.far, self.send_sem = own, far, send_sem
        self.x_recv, self.y_recv, self.rest, self.diag_recv = sems
        self.rows = far.shape[0] // 8
        self.half = self.rows // 2
        self.cols = far.shape[1]
        self.me, _, self.partner, self.x_near, self.y_near, self.diag = places()
        self.runs = runs_of(TAIL_RUNS, self.cols, sum(TAIL_RUNS))

    def send(self, source, at, tall, c, width, recv_sem, peer):
        pltpu.make_async_remote_copy(
            src_ref=block_of(source, at, tall, c, width),
            dst_ref=block_of(self.far, at, tall, c, width),
            send_sem=self.send_sem, recv_sem=recv_sem,
            device_id={"fsdp": peer}, device_id_type=MESH,
        ).start()

    def arrived(self, at, tall, c, width, recv_sem):
        ref = block_of(self.far, at, tall, c, width)
        pltpu.make_async_remote_copy(
            src_ref=ref, dst_ref=ref, send_sem=self.send_sem, recv_sem=recv_sem,
            device_id={"fsdp": self.partner}, device_id_type=MESH,
        ).wait_recv()

    def start(self):
        top = self.me * self.rows
        low = top + self.half
        for r, (c, width) in enumerate(self.runs):
            self.send(
                self.own, top, self.half, c, width, self.x_recv.at[r], self.x_near
            )
            self.send(
                self.own, low, self.half, c, width, self.y_recv.at[r], self.y_near
            )
        self.send(
            self.own, low, self.half, 0, self.cols, self.rest.at[0], self.x_near
        )
        self.send(
            self.own, top, self.half, 0, self.cols, self.rest.at[1], self.y_near
        )

    def take(self, r):
        c, width = self.runs[r]
        top = self.x_near * self.rows
        low = self.y_near * self.rows + self.half
        self.arrived(top, self.half, c, width, self.x_recv.at[r])
        self.arrived(low, self.half, c, width, self.y_recv.at[r])

    def forward(self, r, source):
        c, width = self.runs[r]
        top = self.x_near * self.rows
        low = self.y_near * self.rows + self.half
        self.send(
            source, top, self.half, c, width, self.diag_recv.at[0, r], self.y_near
        )
        self.send(
            source, low, self.half, c, width, self.diag_recv.at[1, r], self.x_near
        )

    def take_rest(self):
        for near, first, sem in (
            (self.x_near, self.half, self.rest.at[0]),
            (self.y_near, 0, self.rest.at[1]),
        ):
            self.arrived(near * self.rows + first, self.half, 0, self.cols, sem)

    def finish(self, r, then):
        c, width = self.runs[r]
        for h in range(2):
            at = self.diag * self.rows + h * self.half
            self.arrived(at, self.half, c, width, self.diag_recv.at[h, r])
            then(at, self.half, c, width)

    def left(self, blocks, c, width):
        ref = block_of(self.far, 0, blocks * self.rows, c, width)
        pltpu.make_async_remote_copy(
            src_ref=ref, dst_ref=ref, send_sem=self.send_sem,
            recv_sem=self.x_recv.at[0], device_id={"fsdp": self.partner},
            device_id_type=MESH,
        ).wait_send()


def gather_kernel(total_rows, *refs):
    ins, gain_ref = refs[:9], refs[9]
    outs, head, tail, factors = refs[10], refs[11], refs[12], refs[13:16]
    (
        bufs, gain_line, gain_buf, parts, early,
        load_sem, gain_sem, sum_send, sum_recv, early_send, early_recv,
        x_recv, y_recv, x_rest, y_rest, diag_recv,
        x_tail, y_tail, rest_tail, diag_tail, tail_send,
        chip_recv, chip_tail, send_sem, chip_send,
    ) = refs[16:]
    w_buf, first_buf, second_buf = (bufs.at[k] for k in range(3))
    rows, cols = bufs.shape[2:]
    half = rows // 2

    me, core, partner, x_near, y_near, diag = places()
    peers = [
        diag + 1 - 2 * core, diag, x_near + 1 - 2 * core, y_near + 1 - 2 * core,
        x_near, y_near, partner,
    ]
    units = units_of(cols)
    count = len(units)
    head_cols = head.shape[1]
    runs = runs_of(HEAD_RUNS, head_cols, sum(HEAD_RUNS))
    early_width = units[0][2]
    early_rows = half * early_width // cols
    head_rows = rows * head_cols // cols

    barrier = pltpu.get_barrier_semaphore()
    for peer in peers:
        pl.semaphore_signal(
            barrier, inc=1, device_id={"fsdp": peer}, device_id_type=MESH
        )

    def load(u):
        if u < count:
            m, c, width = units[u]
            at = pl.ds(c, width)
            for k in range(3):
                pltpu.make_async_copy(
                    ins[3 * m + k].at[:, at], bufs.at[k, m, :, at],
                    load_sem.at[u % 4],
                ).start()

    def loaded(u):
        m, c, width = units[u]
        ref = bufs.at[:, m, :, pl.ds(c, width)]
        pltpu.make_async_copy(ref, ref, load_sem.at[u % 4]).wait()

    gain_copy = pltpu.make_async_copy(gain_ref, gain_line, gain_sem)
    gain_copy.start()
    for u in range(START):
        load(u)

    gain_copy.wait()
    for k in range(rows // 128):
        line = gain_line[:, pl.ds(k * 128, 128)]
        gain_buf[pl.ds(k * 128, 128), :] = jnp.broadcast_to(line, (128, 128)).T

    def sums(u):
        m, c, width = units[u]
        loaded(u)
        if u == 0:
            for v in range(START, AHEAD):
                load(v)
        load(u + AHEAD)
        tiles = width // 128

        def body(i, acc):
            at = pl.ds(pl.multiple_of(i * STEP, STEP), STEP)
            gain = gain_buf[at, :]
            new = []
            for t in range(tiles):
                lanes = pl.ds(c + t * 128, 128)
                hold = hold_rate * first_buf[m, at, lanes] + second_buf[m, at, lanes]
                gained = (w_buf[m, at, lanes] - learn_rate * hold) * gain
                w_buf[m, at, lanes] = gained
                size = jnp.abs(gained)
                new.append(
                    acc[t] + jnp.sum(size.reshape(STEP // 8, 8, 128), axis=0)
                )
            return tuple(new)

        acc = lax.fori_loop(
            0, rows // STEP, body,
            tuple(jnp.zeros((8, 128), jnp.float32) for _ in range(tiles)),
        )
        for t in range(tiles):
            parts[me, m, :, pl.ds(c + t * 128, 128)] = jnp.sum(
                acc[t], axis=0, keepdims=True
            )

    def send_sums(u):
        m, c, width = units[u]
        at = pl.ds(c, width)
        ref = parts.at[me, m, :, at]
        for peer in peers:
            pltpu.make_async_remote_copy(
                src_ref=ref, dst_ref=ref, send_sem=sum_send,
                recv_sem=sum_recv.at[u],
                device_id={"fsdp": peer}, device_id_type=MESH,
            ).start()

    def block(m, owner, first, tall, c, width):
        at = owner * rows + first
        if m == 1:
            at = at + 8 * rows
        if m == 2:
            ref, c = (head, c) if c < head_cols else (tail, c - head_cols)
        else:
            ref = outs
        return block_of(ref, at, tall, c, width)

    def span(tall):
        return outs.at[pl.ds(0, tall), :]

    def send(ref, recv_sem, peer):
        pltpu.make_async_remote_copy(
            src_ref=ref, dst_ref=ref, send_sem=send_sem, recv_sem=recv_sem,
            device_id={"fsdp": peer}, device_id_type=MESH,
        ).start()

    def cross(ref, recv_sem):
        pltpu.make_async_remote_copy(
            src_ref=ref, dst_ref=ref, send_sem=chip_send, recv_sem=recv_sem,
            device_id={"fsdp": partner}, device_id_type=MESH,
        ).start()

    def arrived(ref, recv_sem):
        pltpu.make_async_remote_copy(
            src_ref=ref, dst_ref=ref, send_sem=send_sem, recv_sem=recv_sem,
            device_id={"fsdp": partner}, device_id_type=MESH,
        ).wait_recv()

    def left(ref, sem):
        pltpu.make_async_remote_copy(
            src_ref=ref, dst_ref=ref, send_sem=sem, recv_sem=chip_recv,
            device_id={"fsdp": partner}, device_id_type=MESH,
        ).wait_send()

    def early_copy(side, peer, first, tall):
        at = pl.ds(first, tall)
        return pltpu.make_async_remote_copy(
            src_ref=w_buf.at[0, at, pl.ds(0, early_width)],
            dst_ref=early.at[side, at], send_sem=early_send,
            recv_sem=early_recv.at[side],
            device_id={"fsdp": peer}, device_id_type=MESH,
        )

    def scaled(source, m, owner, lo, hi, c, width):
        scale = jnp.broadcast_to(
            1.0 / factors[m][:, pl.ds(c, width)], (16, width)
        )

        def body(i, carry):
            for k in range(STEP // 16):
                at = pl.multiple_of(i * STEP + k * 16, 16)
                tile = source[pl.ds(at, 16), pl.ds(c, width)] * scale
                block(m, owner, at, 16, c, width)[...] = tile.astype(jnp.bfloat16)
            return carry

        lax.fori_loop(lo // STEP, hi // STEP, body, 0)

    def finish(u):
        m, c, width = units[u]
        at = pl.ds(c, width)
        arrived(parts.at[pl.ds(0, 7), m, :, at], sum_recv.at[u])
        total = parts[0, m, :, at]
        for owner in range(1, 8):
            total = total + parts[owner, m, :, at]
        factors[m][:, at] = total / total_rows
        for h in (1, 0):
            scaled(w_buf.at[m], m, me, h * half, (h + 1) * half, c, width)
            if u == count - 1 or u == 0 and h == 0:
                continue
            ref = block(m, me, h * half, half, c, width)
            send(ref, x_recv.at[m] if h == 0 else x_rest, x_near)
            send(ref, y_recv.at[m] if h == 1 else y_rest, y_near)
        cross(
            block(m, me, 0, rows, c, width),
            chip_tail if u == count - 1 else chip_recv,
        )

    def take_early():
        for side, owner in enumerate((x_near, y_near)):
            arrived(early.at[side], early_recv.at[side])
            scaled(early.at[side], 0, owner, 0, half, 0, early_width)

    sums(0)
    pl.semaphore_wait(barrier, 7)
    send_sums(0)
    early_copy(0, x_near, 0, EARLY).start()
    early_copy(1, y_near, 0, EARLY).start()
    sums(1)
    send_sums(1)
    early_copy(0, x_near, EARLY, half - EARLY).start()
    early_copy(1, y_near, EARLY, half - EARLY).start()
    sums(2)
    send_sums(2)
    finish(0)
    finish(1)
    take_early()
    for u in range(3, count):
        sums(u)
        send_sums(u)
        finish(u - 1)
    finish(count - 1)

    widths = (cols, cols, head_cols)
    pieces = [
        (m, slot, c, width)
        for slot, (m, (c, width)) in enumerate(
            [(0, (0, cols)), (1, (0, cols))] + [(2, run) for run in runs]
        )
    ]
    for m in range(3):
        whole = half * widths[m] // cols
        arrived(span(whole - early_rows * (m == 0)), x_recv.at[m])
        arrived(span(whole), y_recv.at[m])
        for piece, slot, c, width in pieces:
            if piece == m:
                send(
                    block(m, x_near, 0, half, c, width), diag_recv.at[0, slot],
                    y_near,
                )
                send(
                    block(m, y_near, half, half, c, width), diag_recv.at[1, slot],
                    x_near,
                )

    relay = Relay(tail, tail, (x_tail, y_tail, rest_tail, diag_tail), tail_send)

    @pl.when(core == 0)
    def _():
        relay.start()

    arrived(span(2 * half + head_rows // 2), x_rest)
    arrived(span(2 * half + head_rows // 2 - early_rows), y_rest)
    for m in range(3):
        for owner in (x_near, y_near):
            cross(block(m, owner, 0, rows, 0, widths[m]), chip_recv)
    for m, slot, c, width in pieces:
        for h in range(2):
            ref = block(m, diag, h * half, half, c, width)
            arrived(ref, diag_recv.at[h, slot])
            cross(ref, chip_recv)

    @pl.when(core == 0)
    def _():
        for r in range(len(relay.runs)):
            relay.take(r)
            if r < SPLIT:
                relay.forward(r, tail)
        relay.take_rest()
        for r in range(SPLIT):
            relay.finish(r, lambda *at: None)
        relay.left(2, 0, relay.cols)
        relay.left(1, 0, relay.runs[SPLIT][0])

    arrived(span(4 * (2 * rows + head_rows)), chip_recv)
    arrived(tail.at[pl.ds(0, rows), :], chip_tail)
    left(span(3 * (2 * rows + head_rows) - 2 * early_rows), send_sem)
    left(span(4 * (2 * rows + head_rows) + rows - head_rows), chip_send)
    left(parts.at[pl.ds(0, 7)], sum_send)
    left(early, early_send)


def tail_kernel(held, token, value, *sems):
    *relay_sems, relay_send, chip_recv, chip_send, ready = sems
    rows = held.shape[0] // 8
    _, core, partner, x_near, y_near, diag = places()

    barrier = pltpu.get_barrier_semaphore()
    for peer in (x_near, y_near):
        pl.semaphore_signal(
            barrier, inc=1, device_id={"fsdp": peer}, device_id_type=MESH
        )

    @pl.when(core == 1)
    def _():
        pl.semaphore_signal(
            barrier, inc=1, device_id={"fsdp": partner}, device_id_type=MESH
        )

    pl.semaphore_wait(barrier, 3 - core)
    relay = Relay(held, value, relay_sems, relay_send)
    cols = relay.cols
    cut = relay.runs[SPLIT][0]

    def copy_of(source, at, tall, c, width):
        return pltpu.make_async_remote_copy(
            src_ref=block_of(source, at, tall, c, width),
            dst_ref=block_of(value, at, tall, c, width),
            send_sem=chip_send, recv_sem=chip_recv,
            device_id={"fsdp": partner}, device_id_type=MESH,
        )

    @pl.when(core == 0)
    def _():
        pl.semaphore_signal(
            ready, inc=1, device_id={"fsdp": partner}, device_id_type=MESH
        )
        for r in range(SPLIT, len(relay.runs)):
            relay.forward(r, held)
        for owner, width in ((x_near, cols), (y_near, cols), (diag, cut)):
            copy_of(held, owner * rows, rows, 0, width).start()
        for r in range(SPLIT, len(relay.runs)):
            relay.finish(r, lambda *at: copy_of(value, *at).start())
        relay.left(1, cut, cols - cut)

    @pl.when(core == 1)
    def _():
        relay.start()
        for r in range(len(relay.runs)):
            relay.take(r)
            relay.forward(r, value)
        relay.take_rest()
        pl.semaphore_wait(ready, 1)
        for owner in (x_near, y_near):
            copy_of(value, owner * rows, rows, 0, cols).start()
        for r in range(len(relay.runs)):
            relay.finish(r, lambda *at: copy_of(value, *at).start())
        relay.left(3, 0, cols)

    three = copy_of(value, 0, 3 * rows, 0, cols)
    three.wait_recv()
    three.wait_send()


def write_first(src, head, *refs):
    lines, outs, line_outs, sem = refs[:3], refs[3:6], refs[6:9], refs[9]
    copies = [
        pltpu.make_async_copy(lines[k], line_outs[k], sem.at[3 + k])
        for k in range(3)
    ]
    for copy in copies:
        copy.start()
    tall = outs[0].shape[0]
    step = tall // PIECES
    part = pl.ds(0, head.shape[1])
    for p in range(PIECES):
        at = pl.ds(p * step, step)
        for k in range(2):
            pltpu.make_async_copy(
                src.at[pl.ds(k * tall + p * step, step), :], outs[k].at[at, :],
                sem.at[k],
            ).start()
        pltpu.make_async_copy(
            head.at[at, :], outs[2].at[at, part], sem.at[2]
        ).start()
    for k in range(2):
        whole = src.at[pl.ds(k * tall, tall), :]
        pltpu.make_async_copy(whole, outs[k], sem.at[k]).wait()
    pltpu.make_async_copy(head, outs[2].at[:, part], sem.at[2]).wait()
    for copy in copies:
        copy.wait()


def write_last(held, value, first, out, sem):
    rows = out.shape[0] // 8
    width = held.shape[1]
    start = out.shape[1] - width
    cut = runs_of(TAIL_RUNS, width, sum(TAIL_RUNS))[SPLIT][0]
    me, core, _, x_near, y_near, diag = places()
    step = 8 * rows // PIECES

    def put(src, owner, c=0, wide=width):
        for p in range(rows // step):
            at = owner * rows + p * step
            pltpu.make_async_copy(
                block_of(src, at, step, c, wide),
                block_of(out, at, step, start + c, wide), sem,
            ).start()

    for k in range(2):
        put(held, me - core + k)
    for owner in (x_near, y_near, diag):
        put(value, owner + 1 - 2 * core)

    @pl.when(core == 0)
    def _():
        put(held, x_near)
        put(held, y_near)
        put(held, diag, 0, cut)
        put(value, diag, cut, width - cut)

    @pl.when(core == 1)
    def _():
        for owner in (x_near, y_near, diag):
            put(value, owner)

    whole = out.at[:, pl.ds(start, width)]
    pltpu.make_async_copy(value, whole, sem).wait()


def ringed(*args, total_rows):
    rows, cols = args[0].shape
    units = units_of(cols)
    count = len(units)
    vmem = pl.BlockSpec(memory_space=pltpu.VMEM)
    hbm = pl.BlockSpec(memory_space=pltpu.HBM)
    dma = pltpu.SemaphoreType.DMA
    tail_cols = units[-1][2]
    head = pltpu.VMEM((8 * rows, cols - tail_cols), jnp.bfloat16)
    tail = pltpu.VMEM((8 * rows, tail_cols), jnp.bfloat16)
    line = jax.ShapeDtypeStruct((1, cols), jnp.float32)
    runs = len(TAIL_RUNS)
    slots = 2 + len(HEAD_RUNS)
    relay = [dma((runs,)), dma((runs,)), dma((2,)), dma((2, runs)), dma]
    pair, head, held, *factors = pl.pallas_call(
        functools.partial(gather_kernel, total_rows),
        out_shape=[pltpu.VMEM((16 * rows, cols), jnp.bfloat16), head, tail]
        + [pltpu.VMEM((1, cols), jnp.float32)] * 3,
        in_specs=[hbm] * 10,
        out_specs=[vmem] * 6,
        scratch_shapes=[
            pltpu.VMEM((3, 3, rows, cols), jnp.float32),
            pltpu.VMEM((1, rows), jnp.float32),
            pltpu.VMEM((rows, 128), jnp.float32),
            pltpu.VMEM((8, 3, 1, cols), jnp.float32),
            pltpu.VMEM((2, rows // 2, units[0][2]), jnp.float32),
            dma((4,)), dma, dma, dma((count,)), dma, dma((2,)),
            dma((3,)), dma((3,)), dma, dma, dma((2, slots)),
            *relay, dma, dma, dma, dma,
        ],
        compiler_params=pltpu.CompilerParams(
            collective_id=0, has_side_effects=True,
            vmem_limit_bytes=VMEM_BYTES - 3 * 16 * rows * cols - 2**20,
        ),
        name="gather",
    )(*(
        pltpu.with_memory_space_constraint(a, pltpu.HBM)
        for a in (*args[:9], args[9].reshape(1, rows))
    ))
    ready = jax.ShapeDtypeStruct((8 * rows, cols), jnp.bfloat16)
    query, key, first, *lines = pl.pallas_call(
        write_first,
        out_shape=[ready] * 2 + [pltpu.HBM(ready.shape, ready.dtype)] + [line] * 3,
        in_specs=[vmem] * 5,
        out_specs=[hbm] * 6,
        scratch_shapes=[dma((6,))],
        compiler_params=pltpu.CompilerParams(
            has_side_effects=True, vmem_limit_bytes=2**20
        ),
        name="write_first",
    )(pair, head, *factors)
    value = pl.pallas_call(
        tail_kernel,
        out_shape=tail,
        in_specs=[vmem, hbm],
        out_specs=vmem,
        scratch_shapes=[*relay, dma, dma, pltpu.SemaphoreType.REGULAR],
        compiler_params=pltpu.CompilerParams(
            collective_id=1, has_side_effects=True, vmem_limit_bytes=2**20
        ),
        name="tail",
    )(held, pltpu.with_memory_space_constraint(lines[0], pltpu.HBM))
    value = pl.pallas_call(
        write_last,
        out_shape=pltpu.HBM(ready.shape, ready.dtype),
        in_specs=[vmem, vmem, hbm],
        out_specs=hbm,
        scratch_shapes=[dma],
        input_output_aliases={2: 0},
        compiler_params=pltpu.CompilerParams(vmem_limit_bytes=2**20),
        name="write_last",
    )(held, value, pltpu.with_memory_space_constraint(first, pltpu.HBM))
    return [query, key, value] + [f.reshape(cols) for f in lines]


def on_device(*args, devices):
    rows, cols = args[0].shape
    total_rows = devices * rows
    fits = rows * cols * (36 + 48) <= 48 * 2**20
    if devices == 8 and rows % 128 == 0 and cols % (128 * UNITS) == 0 and fits:
        return tuple(ringed(*args, total_rows=total_rows))
    return plain(*args, rows=total_rows)


def solution(mesh):
    return jax.shard_map(
        functools.partial(on_device, devices=mesh.shape["fsdp"]),
        mesh=mesh,
        in_specs=(P("fsdp", "model"),) * 9 + (P("fsdp"),),
        out_specs=(P(None, "model"),) * 3 + (P("model"),) * 3,
        check_vma=False,
    )
```

```python
import functools
import math

import jax
import jax.numpy as jnp
from jax import lax
from jax.experimental import pallas as pl
from jax.experimental.pallas import tpu as pltpu
from jax.sharding import PartitionSpec as P

learn_rate = 0.2
hold_rate = 0.9
MESH = pl.DeviceIdType.MESH
UNITS = 8
PARTS = ((1, 2, 5), (8,), (2, 6))
HEAD_RUNS = (1, 1)
TAIL_RUNS = (2, 2, 1, 1)
SPLIT = 3
EARLY = 96
STEP = 32
AHEAD = 2
PIECES = 32
VMEM_BYTES = 67_043_328


def plain(
    w_query,
    first_query,
    second_query,
    w_key,
    first_key,
    second_key,
    w_value,
    first_value,
    second_value,
    norm_gain,
    rows,
):
    gained = []
    for w, first, second in (
        (w_query, first_query, second_query),
        (w_key, first_key, second_key),
        (w_value, first_value, second_value),
    ):
        hold = hold_rate * first + second
        gained.append((w - learn_rate * hold) * norm_gain[:, None])
    totals = lax.psum(tuple(jnp.sum(jnp.abs(g), axis=0) for g in gained), "fsdp")
    factors = tuple(t / rows for t in totals)
    ready = tuple(
        lax.all_gather(
            (g / f).astype(jnp.bfloat16), "fsdp", axis=0, tiled=True
        )
        for g, f in zip(gained, factors)
    )
    return ready + factors


def units_of(cols):
    units = []
    for m, sizes in enumerate(PARTS):
        first = 0
        for size in sizes:
            units.append((m, first, size * cols // UNITS))
            first += size * cols // UNITS
    return units


def runs_of(sizes, cols, parts):
    runs = []
    first = 0
    for size in sizes:
        runs.append((first, size * cols // parts))
        first += size * cols // parts
    return runs


def places():
    me = lax.axis_index("fsdp")
    core = me % 2
    x = (me // 2) % 2
    y = me // 4
    partner = me + 1 - 2 * core
    x_near = me + 2 - 4 * x
    y_near = me + 4 - 8 * y
    diag = x_near + 4 - 8 * y
    return me, core, partner, x_near, y_near, diag


def block_of(ref, at, tall, c, width):
    return ref.at[pl.ds(pl.multiple_of(at, 16), tall), pl.ds(c, width)]


class Relay:
    def __init__(self, own, far, sems, send_sem):
        self.own, self.far, self.send_sem = own, far, send_sem
        self.x_recv, self.y_recv, self.rest, self.diag_recv = sems
        self.rows = far.shape[0] // 8
        self.half = self.rows // 2
        self.cols = far.shape[1]
        self.me, _, self.partner, self.x_near, self.y_near, self.diag = places()
        self.runs = runs_of(TAIL_RUNS, self.cols, sum(TAIL_RUNS))

    def send(self, source, at, tall, c, width, recv_sem, peer):
        pltpu.make_async_remote_copy(
            src_ref=block_of(source, at, tall, c, width),
            dst_ref=block_of(self.far, at, tall, c, width),
            send_sem=self.send_sem, recv_sem=recv_sem,
            device_id={"fsdp": peer}, device_id_type=MESH,
        ).start()

    def arrived(self, at, tall, c, width, recv_sem):
        ref = block_of(self.far, at, tall, c, width)
        pltpu.make_async_remote_copy(
            src_ref=ref, dst_ref=ref, send_sem=self.send_sem, recv_sem=recv_sem,
            device_id={"fsdp": self.partner}, device_id_type=MESH,
        ).wait_recv()

    def start(self):
        top = self.me * self.rows
        low = top + self.half
        for r, (c, width) in enumerate(self.runs):
            self.send(
                self.own, top, self.half, c, width, self.x_recv.at[r], self.x_near
            )
            self.send(
                self.own, low, self.half, c, width, self.y_recv.at[r], self.y_near
            )
        self.send(
            self.own, low, self.half, 0, self.cols, self.rest.at[0], self.x_near
        )
        self.send(
            self.own, top, self.half, 0, self.cols, self.rest.at[1], self.y_near
        )

    def take(self, r):
        c, width = self.runs[r]
        top = self.x_near * self.rows
        low = self.y_near * self.rows + self.half
        self.arrived(top, self.half, c, width, self.x_recv.at[r])
        self.arrived(low, self.half, c, width, self.y_recv.at[r])

    def forward(self, r, source):
        c, width = self.runs[r]
        top = self.x_near * self.rows
        low = self.y_near * self.rows + self.half
        self.send(
            source, top, self.half, c, width, self.diag_recv.at[0, r], self.y_near
        )
        self.send(
            source, low, self.half, c, width, self.diag_recv.at[1, r], self.x_near
        )

    def take_rest(self):
        for near, first, sem in (
            (self.x_near, self.half, self.rest.at[0]),
            (self.y_near, 0, self.rest.at[1]),
        ):
            self.arrived(near * self.rows + first, self.half, 0, self.cols, sem)

    def finish(self, r, then):
        c, width = self.runs[r]
        for h in range(2):
            at = self.diag * self.rows + h * self.half
            self.arrived(at, self.half, c, width, self.diag_recv.at[h, r])
            then(at, self.half, c, width)

    def left(self, blocks, c, width):
        ref = block_of(self.far, 0, blocks * self.rows, c, width)
        pltpu.make_async_remote_copy(
            src_ref=ref, dst_ref=ref, send_sem=self.send_sem,
            recv_sem=self.x_recv.at[0], device_id={"fsdp": self.partner},
            device_id_type=MESH,
        ).wait_send()


def gather_kernel(total_rows, *refs):
    ins, gain_ref = refs[:9], refs[9]
    outs, head, tail, factors = refs[10], refs[11], refs[12], refs[13:16]
    (
        bufs, gain_line, gain_buf, parts, early,
        load_sem, gain_sem, sum_send, sum_recv, early_send, early_recv,
        x_recv, y_recv, x_rest, y_rest, diag_recv,
        x_tail, y_tail, rest_tail, diag_tail, tail_send,
        chip_recv, chip_tail, send_sem, chip_send,
    ) = refs[16:]
    w_buf, first_buf, second_buf = (bufs.at[k] for k in range(3))
    rows, cols = bufs.shape[2:]
    half = rows // 2

    me, core, partner, x_near, y_near, diag = places()
    peers = [
        diag + 1 - 2 * core, diag, x_near + 1 - 2 * core, y_near + 1 - 2 * core,
        x_near, y_near, partner,
    ]
    units = units_of(cols)
    count = len(units)
    head_cols = head.shape[1]
    runs = runs_of(HEAD_RUNS, head_cols, sum(HEAD_RUNS))
    early_width = units[0][2]
    early_rows = half * early_width // cols
    head_rows = rows * head_cols // cols

    barrier = pltpu.get_barrier_semaphore()
    for peer in peers:
        pl.semaphore_signal(
            barrier, inc=1, device_id={"fsdp": peer}, device_id_type=MESH
        )

    def load(u):
        if u < count:
            m, c, width = units[u]
            at = pl.ds(c, width)
            for k in range(3):
                pltpu.make_async_copy(
                    ins[3 * m + k].at[:, at], bufs.at[k, m, :, at],
                    load_sem.at[u % 2],
                ).start()

    def loaded(u):
        m, c, width = units[u]
        ref = bufs.at[:, m, :, pl.ds(c, width)]
        pltpu.make_async_copy(ref, ref, load_sem.at[u % 2]).wait()

    gain_copy = pltpu.make_async_copy(gain_ref, gain_line, gain_sem)
    gain_copy.start()
    load(0)

    gain_copy.wait()
    load(1)
    for k in range(rows // 128):
        line = gain_line[:, pl.ds(k * 128, 128)]
        gain_buf[pl.ds(k * 128, 128), :] = jnp.broadcast_to(line, (128, 128)).T

    def sums(u):
        m, c, width = units[u]
        loaded(u)
        load(u + AHEAD)
        tiles = width // 128

        def body(i, acc):
            at = pl.ds(pl.multiple_of(i * STEP, STEP), STEP)
            gain = gain_buf[at, :]
            new = []
            for t in range(tiles):
                lanes = pl.ds(c + t * 128, 128)
                hold = hold_rate * first_buf[m, at, lanes] + second_buf[m, at, lanes]
                gained = (w_buf[m, at, lanes] - learn_rate * hold) * gain
                w_buf[m, at, lanes] = gained
                size = jnp.abs(gained)
                new.append(
                    acc[t] + jnp.sum(size.reshape(STEP // 8, 8, 128), axis=0)
                )
            return tuple(new)

        acc = lax.fori_loop(
            0, rows // STEP, body,
            tuple(jnp.zeros((8, 128), jnp.float32) for _ in range(tiles)),
        )
        for t in range(tiles):
            parts[me, m, :, pl.ds(c + t * 128, 128)] = jnp.sum(
                acc[t], axis=0, keepdims=True
            )

    def send_sums(u):
        m, c, width = units[u]
        at = pl.ds(c, width)
        ref = parts.at[me, m, :, at]
        for peer in peers:
            pltpu.make_async_remote_copy(
                src_ref=ref, dst_ref=ref, send_sem=sum_send,
                recv_sem=sum_recv.at[u],
                device_id={"fsdp": peer}, device_id_type=MESH,
            ).start()

    def block(m, owner, first, tall, c, width):
        at = owner * rows + first
        if m == 1:
            at = at + 8 * rows
        if m == 2:
            ref, c = (head, c) if c < head_cols else (tail, c - head_cols)
        else:
            ref = outs
        return block_of(ref, at, tall, c, width)

    def span(tall):
        return outs.at[pl.ds(0, tall), :]

    def send(ref, recv_sem, peer):
        pltpu.make_async_remote_copy(
            src_ref=ref, dst_ref=ref, send_sem=send_sem, recv_sem=recv_sem,
            device_id={"fsdp": peer}, device_id_type=MESH,
        ).start()

    def cross(ref, recv_sem):
        pltpu.make_async_remote_copy(
            src_ref=ref, dst_ref=ref, send_sem=chip_send, recv_sem=recv_sem,
            device_id={"fsdp": partner}, device_id_type=MESH,
        ).start()

    def arrived(ref, recv_sem):
        pltpu.make_async_remote_copy(
            src_ref=ref, dst_ref=ref, send_sem=send_sem, recv_sem=recv_sem,
            device_id={"fsdp": partner}, device_id_type=MESH,
        ).wait_recv()

    def left(ref, sem):
        pltpu.make_async_remote_copy(
            src_ref=ref, dst_ref=ref, send_sem=sem, recv_sem=chip_recv,
            device_id={"fsdp": partner}, device_id_type=MESH,
        ).wait_send()

    def early_copy(side, peer, first, tall):
        at = pl.ds(first, tall)
        return pltpu.make_async_remote_copy(
            src_ref=w_buf.at[0, at, pl.ds(0, early_width)],
            dst_ref=early.at[side, at], send_sem=early_send,
            recv_sem=early_recv.at[side],
            device_id={"fsdp": peer}, device_id_type=MESH,
        )

    def scaled(source, m, owner, lo, hi, c, width):
        scale = jnp.broadcast_to(
            1.0 / factors[m][:, pl.ds(c, width)], (16, width)
        )

        def body(i, carry):
            for k in range(STEP // 16):
                at = pl.multiple_of(i * STEP + k * 16, 16)
                tile = source[pl.ds(at, 16), pl.ds(c, width)] * scale
                block(m, owner, at, 16, c, width)[...] = tile.astype(jnp.bfloat16)
            return carry

        lax.fori_loop(lo // STEP, hi // STEP, body, 0)

    def finish(u):
        m, c, width = units[u]
        at = pl.ds(c, width)
        arrived(parts.at[pl.ds(0, 7), m, :, at], sum_recv.at[u])
        total = parts[0, m, :, at]
        for owner in range(1, 8):
            total = total + parts[owner, m, :, at]
        factors[m][:, at] = total / total_rows
        for h in (1, 0):
            scaled(w_buf.at[m], m, me, h * half, (h + 1) * half, c, width)
            if u == count - 1 or u == 0 and h == 0:
                continue
            ref = block(m, me, h * half, half, c, width)
            send(ref, x_recv.at[m] if h == 0 else x_rest, x_near)
            send(ref, y_recv.at[m] if h == 1 else y_rest, y_near)
        cross(
            block(m, me, 0, rows, c, width),
            chip_tail if u == count - 1 else chip_recv,
        )

    def take_early():
        for side, owner in enumerate((x_near, y_near)):
            arrived(early.at[side], early_recv.at[side])
            scaled(early.at[side], 0, owner, 0, half, 0, early_width)

    sums(0)
    pl.semaphore_wait(barrier, 7)
    send_sums(0)
    early_copy(0, x_near, 0, EARLY).start()
    early_copy(1, y_near, 0, EARLY).start()
    sums(1)
    send_sums(1)
    early_copy(0, x_near, EARLY, half - EARLY).start()
    early_copy(1, y_near, EARLY, half - EARLY).start()
    sums(2)
    send_sums(2)
    finish(0)
    finish(1)
    take_early()
    for u in range(3, count):
        sums(u)
        send_sums(u)
        finish(u - 1)
    finish(count - 1)

    widths = (cols, cols, head_cols)
    pieces = [
        (m, slot, c, width)
        for slot, (m, (c, width)) in enumerate(
            [(0, (0, cols)), (1, (0, cols))] + [(2, run) for run in runs]
        )
    ]
    for m in range(3):
        whole = half * widths[m] // cols
        arrived(span(whole - early_rows * (m == 0)), x_recv.at[m])
        arrived(span(whole), y_recv.at[m])
        for piece, slot, c, width in pieces:
            if piece == m:
                send(
                    block(m, x_near, 0, half, c, width), diag_recv.at[0, slot],
                    y_near,
                )
                send(
                    block(m, y_near, half, half, c, width), diag_recv.at[1, slot],
                    x_near,
                )

    relay = Relay(tail, tail, (x_tail, y_tail, rest_tail, diag_tail), tail_send)

    @pl.when(core == 0)
    def _():
        relay.start()

    arrived(span(2 * half + head_rows // 2), x_rest)
    arrived(span(2 * half + head_rows // 2 - early_rows), y_rest)
    for m in range(3):
        for owner in (x_near, y_near):
            cross(block(m, owner, 0, rows, 0, widths[m]), chip_recv)
    for m, slot, c, width in pieces:
        for h in range(2):
            ref = block(m, diag, h * half, half, c, width)
            arrived(ref, diag_recv.at[h, slot])
            cross(ref, chip_recv)

    @pl.when(core == 0)
    def _():
        for r in range(len(relay.runs)):
            relay.take(r)
            if r < SPLIT:
                relay.forward(r, tail)
        relay.take_rest()
        for r in range(SPLIT):
            relay.finish(r, lambda *at: None)
        relay.left(2, 0, relay.cols)
        relay.left(1, 0, relay.runs[SPLIT][0])

    arrived(span(4 * (2 * rows + head_rows)), chip_recv)
    arrived(tail.at[pl.ds(0, rows), :], chip_tail)
    left(span(3 * (2 * rows + head_rows) - 2 * early_rows), send_sem)
    left(span(4 * (2 * rows + head_rows) + rows - head_rows), chip_send)
    left(parts.at[pl.ds(0, 7)], sum_send)
    left(early, early_send)


def tail_kernel(held, token, value, *sems):
    *relay_sems, relay_send, chip_recv, chip_send, ready = sems
    rows = held.shape[0] // 8
    _, core, partner, x_near, y_near, diag = places()

    barrier = pltpu.get_barrier_semaphore()
    for peer in (x_near, y_near):
        pl.semaphore_signal(
            barrier, inc=1, device_id={"fsdp": peer}, device_id_type=MESH
        )

    @pl.when(core == 1)
    def _():
        pl.semaphore_signal(
            barrier, inc=1, device_id={"fsdp": partner}, device_id_type=MESH
        )

    pl.semaphore_wait(barrier, 3 - core)
    relay = Relay(held, value, relay_sems, relay_send)
    cols = relay.cols
    cut = relay.runs[SPLIT][0]

    def copy_of(source, at, tall, c, width):
        return pltpu.make_async_remote_copy(
            src_ref=block_of(source, at, tall, c, width),
            dst_ref=block_of(value, at, tall, c, width),
            send_sem=chip_send, recv_sem=chip_recv,
            device_id={"fsdp": partner}, device_id_type=MESH,
        )

    @pl.when(core == 0)
    def _():
        pl.semaphore_signal(
            ready, inc=1, device_id={"fsdp": partner}, device_id_type=MESH
        )
        for r in range(SPLIT, len(relay.runs)):
            relay.forward(r, held)
        for owner, width in ((x_near, cols), (y_near, cols), (diag, cut)):
            copy_of(held, owner * rows, rows, 0, width).start()
        for r in range(SPLIT, len(relay.runs)):
            relay.finish(r, lambda *at: copy_of(value, *at).start())
        relay.left(1, cut, cols - cut)

    @pl.when(core == 1)
    def _():
        relay.start()
        for r in range(len(relay.runs)):
            relay.take(r)
            relay.forward(r, value)
        relay.take_rest()
        pl.semaphore_wait(ready, 1)
        for owner in (x_near, y_near):
            copy_of(value, owner * rows, rows, 0, cols).start()
        for r in range(len(relay.runs)):
            relay.finish(r, lambda *at: copy_of(value, *at).start())
        relay.left(3, 0, cols)

    three = copy_of(value, 0, 3 * rows, 0, cols)
    three.wait_recv()
    three.wait_send()


def write_first(src, head, held, *refs):
    lines, outs, line_outs, sem = refs[:3], refs[3:6], refs[6:9], refs[9]
    copies = [
        pltpu.make_async_copy(lines[k], line_outs[k], sem.at[3 + k])
        for k in range(3)
    ]
    for copy in copies:
        copy.start()
    tall = outs[0].shape[0]
    step = tall // PIECES
    width = head.shape[1]
    part = pl.ds(0, width)
    rows = tall // 8
    me, core, *_ = places()
    for p in range(PIECES):
        at = pl.ds(p * step, step)
        for k in range(2):
            pltpu.make_async_copy(
                src.at[pl.ds(k * tall + p * step, step), :], outs[k].at[at, :],
                sem.at[k],
            ).start()
        pltpu.make_async_copy(
            head.at[at, :], outs[2].at[at, part], sem.at[2]
        ).start()
    own = pl.ds(pl.multiple_of((me - core) * rows, 16), 2 * rows)
    rest = pl.ds(width, held.shape[1])
    pair = pltpu.make_async_copy(
        held.at[own, :], outs[2].at[own, rest], sem.at[6]
    )
    pair.start()
    for k in range(2):
        whole = src.at[pl.ds(k * tall, tall), :]
        pltpu.make_async_copy(whole, outs[k], sem.at[k]).wait()
    pair.wait()
    pltpu.make_async_copy(head, outs[2].at[:, part], sem.at[2]).wait()
    for copy in copies:
        copy.wait()


def write_last(held, value, first, out, sem):
    rows = out.shape[0] // 8
    width = held.shape[1]
    start = out.shape[1] - width
    cut = runs_of(TAIL_RUNS, width, sum(TAIL_RUNS))[SPLIT][0]
    _, core, _, x_near, y_near, diag = places()
    step = 8 * rows // PIECES

    def put(src, owner, c=0, wide=width):
        for p in range(rows // step):
            at = owner * rows + p * step
            pltpu.make_async_copy(
                block_of(src, at, step, c, wide),
                block_of(out, at, step, start + c, wide), sem,
            ).start()

    for owner in (x_near, y_near, diag):
        put(value, owner + 1 - 2 * core)

    @pl.when(core == 0)
    def _():
        put(held, x_near)
        put(held, y_near)
        put(held, diag, 0, cut)
        put(value, diag, cut, width - cut)

    @pl.when(core == 1)
    def _():
        for owner in (x_near, y_near, diag):
            put(value, owner)

    six = pl.ds(0, 6 * rows)
    whole = out.at[six, pl.ds(start, width)]
    pltpu.make_async_copy(value.at[six, :], whole, sem).wait()


def ringed(*args, total_rows):
    rows, cols = args[0].shape
    units = units_of(cols)
    count = len(units)
    vmem = pl.BlockSpec(memory_space=pltpu.VMEM)
    hbm = pl.BlockSpec(memory_space=pltpu.HBM)
    dma = pltpu.SemaphoreType.DMA
    tail_cols = units[-1][2]
    head = pltpu.VMEM((8 * rows, cols - tail_cols), jnp.bfloat16)
    tail = pltpu.VMEM((8 * rows, tail_cols), jnp.bfloat16)
    line = jax.ShapeDtypeStruct((1, cols), jnp.float32)
    runs = len(TAIL_RUNS)
    slots = 2 + len(HEAD_RUNS)
    relay = [dma((runs,)), dma((runs,)), dma((2,)), dma((2, runs)), dma]
    pair, head, held, *factors = pl.pallas_call(
        functools.partial(gather_kernel, total_rows),
        out_shape=[pltpu.VMEM((16 * rows, cols), jnp.bfloat16), head, tail]
        + [pltpu.VMEM((1, cols), jnp.float32)] * 3,
        in_specs=[hbm] * 10,
        out_specs=[vmem] * 6,
        scratch_shapes=[
            pltpu.VMEM((3, 3, rows, cols), jnp.float32),
            pltpu.VMEM((1, rows), jnp.float32),
            pltpu.VMEM((rows, 128), jnp.float32),
            pltpu.VMEM((8, 3, 1, cols), jnp.float32),
            pltpu.VMEM((2, rows // 2, units[0][2]), jnp.float32),
            dma((2,)), dma, dma, dma((count,)), dma, dma((2,)),
            dma((3,)), dma((3,)), dma, dma, dma((2, slots)),
            *relay, dma, dma, dma, dma,
        ],
        compiler_params=pltpu.CompilerParams(
            collective_id=0, has_side_effects=True,
            vmem_limit_bytes=VMEM_BYTES - 3 * 16 * rows * cols - 2**20,
        ),
        name="gather",
    )(*(
        pltpu.with_memory_space_constraint(a, pltpu.HBM)
        for a in (*args[:9], args[9].reshape(1, rows))
    ))
    ready = jax.ShapeDtypeStruct((8 * rows, cols), jnp.bfloat16)
    query, key, first, *lines = pl.pallas_call(
        write_first,
        out_shape=[ready] * 2 + [pltpu.HBM(ready.shape, ready.dtype)] + [line] * 3,
        in_specs=[vmem] * 6,
        out_specs=[hbm] * 6,
        scratch_shapes=[dma((7,))],
        compiler_params=pltpu.CompilerParams(
            has_side_effects=True, vmem_limit_bytes=2**20
        ),
        name="write_first",
    )(pair, head, held, *factors)
    value = pl.pallas_call(
        tail_kernel,
        out_shape=tail,
        in_specs=[vmem, hbm],
        out_specs=vmem,
        scratch_shapes=[*relay, dma, dma, pltpu.SemaphoreType.REGULAR],
        compiler_params=pltpu.CompilerParams(
            collective_id=1, has_side_effects=True, vmem_limit_bytes=2**20
        ),
        name="tail",
    )(held, pltpu.with_memory_space_constraint(lines[0], pltpu.HBM))
    value = pl.pallas_call(
        write_last,
        out_shape=pltpu.HBM(ready.shape, ready.dtype),
        in_specs=[vmem, vmem, hbm],
        out_specs=hbm,
        scratch_shapes=[dma],
        input_output_aliases={2: 0},
        compiler_params=pltpu.CompilerParams(vmem_limit_bytes=2**20),
        name="write_last",
    )(held, value, pltpu.with_memory_space_constraint(first, pltpu.HBM))
    return [query, key, value] + [f.reshape(cols) for f in lines]


def on_device(*args, devices):
    rows, cols = args[0].shape
    total_rows = devices * rows
    fits = rows * cols * (36 + 48) <= 48 * 2**20
    if devices == 8 and rows % 128 == 0 and cols % (128 * UNITS) == 0 and fits:
        return tuple(ringed(*args, total_rows=total_rows))
    return plain(*args, rows=total_rows)


def solution(mesh):
    return jax.shard_map(
        functools.partial(on_device, devices=mesh.shape["fsdp"]),
        mesh=mesh,
        in_specs=(P("fsdp", "model"),) * 9 + (P("fsdp"),),
        out_specs=(P(None, "model"),) * 3 + (P("model"),) * 3,
        check_vma=False,
    )
```

```python
import functools
import math

import jax
import jax.numpy as jnp
from jax import lax
from jax.experimental import pallas as pl
from jax.experimental.pallas import tpu as pltpu
from jax.sharding import PartitionSpec as P

learn_rate = 0.2
hold_rate = 0.9
MESH = pl.DeviceIdType.MESH
UNITS = 8
PARTS = ((1, 2, 5), (8,), (2, 6))
HEAD_RUNS = (1, 1)
TAIL_RUNS = (2, 2, 1, 1)
SPLIT = 3
DIRECT = 2
EARLY = 96
STEP = 32
AHEAD = 2
PIECES = 32
VMEM_BYTES = 67_043_328


def plain(
    w_query,
    first_query,
    second_query,
    w_key,
    first_key,
    second_key,
    w_value,
    first_value,
    second_value,
    norm_gain,
    rows,
):
    gained = []
    for w, first, second in (
        (w_query, first_query, second_query),
        (w_key, first_key, second_key),
        (w_value, first_value, second_value),
    ):
        hold = hold_rate * first + second
        gained.append((w - learn_rate * hold) * norm_gain[:, None])
    totals = lax.psum(tuple(jnp.sum(jnp.abs(g), axis=0) for g in gained), "fsdp")
    factors = tuple(t / rows for t in totals)
    ready = tuple(
        lax.all_gather(
            (g / f).astype(jnp.bfloat16), "fsdp", axis=0, tiled=True
        )
        for g, f in zip(gained, factors)
    )
    return ready + factors


def units_of(cols):
    units = []
    for m, sizes in enumerate(PARTS):
        first = 0
        for size in sizes:
            units.append((m, first, size * cols // UNITS))
            first += size * cols // UNITS
    return units


def runs_of(sizes, cols, parts):
    runs = []
    first = 0
    for size in sizes:
        runs.append((first, size * cols // parts))
        first += size * cols // parts
    return runs


def places():
    me = lax.axis_index("fsdp")
    core = me % 2
    x = (me // 2) % 2
    y = me // 4
    partner = me + 1 - 2 * core
    x_near = me + 2 - 4 * x
    y_near = me + 4 - 8 * y
    diag = x_near + 4 - 8 * y
    return me, core, partner, x_near, y_near, diag


def block_of(ref, at, tall, c, width):
    return ref.at[pl.ds(pl.multiple_of(at, 16), tall), pl.ds(c, width)]


class Relay:
    def __init__(self, own, far, sems, send_sem):
        self.own, self.far, self.send_sem = own, far, send_sem
        self.x_recv, self.y_recv, self.rest, self.diag_recv = sems
        self.rows = far.shape[0] // 8
        self.half = self.rows // 2
        self.cols = far.shape[1]
        self.me, _, self.partner, self.x_near, self.y_near, self.diag = places()
        self.runs = runs_of(TAIL_RUNS, self.cols, sum(TAIL_RUNS))

    def send(self, source, at, tall, c, width, recv_sem, peer):
        pltpu.make_async_remote_copy(
            src_ref=block_of(source, at, tall, c, width),
            dst_ref=block_of(self.far, at, tall, c, width),
            send_sem=self.send_sem, recv_sem=recv_sem,
            device_id={"fsdp": peer}, device_id_type=MESH,
        ).start()

    def arrived(self, at, tall, c, width, recv_sem):
        ref = block_of(self.far, at, tall, c, width)
        pltpu.make_async_remote_copy(
            src_ref=ref, dst_ref=ref, send_sem=self.send_sem, recv_sem=recv_sem,
            device_id={"fsdp": self.partner}, device_id_type=MESH,
        ).wait_recv()

    def start(self):
        top = self.me * self.rows
        low = top + self.half
        for r, (c, width) in enumerate(self.runs):
            self.send(
                self.own, top, self.half, c, width, self.x_recv.at[r], self.x_near
            )
            self.send(
                self.own, low, self.half, c, width, self.y_recv.at[r], self.y_near
            )
        self.send(
            self.own, low, self.half, 0, self.cols, self.rest.at[0], self.x_near
        )
        self.send(
            self.own, top, self.half, 0, self.cols, self.rest.at[1], self.y_near
        )

    def take(self, r):
        c, width = self.runs[r]
        top = self.x_near * self.rows
        low = self.y_near * self.rows + self.half
        self.arrived(top, self.half, c, width, self.x_recv.at[r])
        self.arrived(low, self.half, c, width, self.y_recv.at[r])

    def forward(self, r, source):
        c, width = self.runs[r]
        top = self.x_near * self.rows
        low = self.y_near * self.rows + self.half
        self.send(
            source, top, self.half, c, width, self.diag_recv.at[0, r], self.y_near
        )
        self.send(
            source, low, self.half, c, width, self.diag_recv.at[1, r], self.x_near
        )

    def take_rest(self):
        for near, first, sem in (
            (self.x_near, self.half, self.rest.at[0]),
            (self.y_near, 0, self.rest.at[1]),
        ):
            self.arrived(near * self.rows + first, self.half, 0, self.cols, sem)

    def finish(self, r, then):
        c, width = self.runs[r]
        for h in range(2):
            at = self.diag * self.rows + h * self.half
            self.arrived(at, self.half, c, width, self.diag_recv.at[h, r])
            then(at, self.half, c, width)

    def left(self, blocks, c, width):
        ref = block_of(self.far, 0, blocks * self.rows, c, width)
        pltpu.make_async_remote_copy(
            src_ref=ref, dst_ref=ref, send_sem=self.send_sem,
            recv_sem=self.x_recv.at[0], device_id={"fsdp": self.partner},
            device_id_type=MESH,
        ).wait_send()


def gather_kernel(total_rows, *refs):
    ins, gain_ref = refs[:9], refs[9]
    outs, head, tail, factors = refs[10], refs[11], refs[12], refs[13:16]
    (
        bufs, gain_line, gain_buf, parts, pair, early,
        load_sem, gain_sem, sum_send, sum_recv, pair_recv, early_send, early_recv,
        x_recv, y_recv, x_rest, y_rest, diag_recv,
        x_tail, y_tail, rest_tail, diag_tail, tail_send,
        chip_recv, chip_tail, send_sem, chip_send,
    ) = refs[16:]
    w_buf, first_buf, second_buf = (bufs.at[k] for k in range(3))
    rows, cols = bufs.shape[2:]
    half = rows // 2

    me, core, partner, x_near, y_near, diag = places()
    peers = [
        diag + 1 - 2 * core, diag, x_near + 1 - 2 * core, y_near + 1 - 2 * core,
        x_near, y_near, partner,
    ]
    units = units_of(cols)
    count = len(units)
    head_cols = head.shape[1]
    runs = runs_of(HEAD_RUNS, head_cols, sum(HEAD_RUNS))
    early_width = units[0][2]
    early_rows = half * early_width // cols
    head_rows = rows * head_cols // cols

    barrier = pltpu.get_barrier_semaphore()
    for peer in peers:
        pl.semaphore_signal(
            barrier, inc=1, device_id={"fsdp": peer}, device_id_type=MESH
        )

    def load(u):
        if u < count:
            m, c, width = units[u]
            at = pl.ds(c, width)
            for k in range(3):
                pltpu.make_async_copy(
                    ins[3 * m + k].at[:, at], bufs.at[k, m, :, at],
                    load_sem.at[u % 2],
                ).start()

    def loaded(u):
        m, c, width = units[u]
        ref = bufs.at[:, m, :, pl.ds(c, width)]
        pltpu.make_async_copy(ref, ref, load_sem.at[u % 2]).wait()

    gain_copy = pltpu.make_async_copy(gain_ref, gain_line, gain_sem)
    gain_copy.start()
    load(0)

    gain_copy.wait()
    load(1)
    for k in range(rows // 128):
        line = gain_line[:, pl.ds(k * 128, 128)]
        gain_buf[pl.ds(k * 128, 128), :] = jnp.broadcast_to(line, (128, 128)).T

    def sums(u):
        m, c, width = units[u]
        loaded(u)
        load(u + AHEAD)
        tiles = width // 128

        def body(i, acc):
            at = pl.ds(pl.multiple_of(i * STEP, STEP), STEP)
            gain = gain_buf[at, :]
            new = []
            for t in range(tiles):
                lanes = pl.ds(c + t * 128, 128)
                hold = hold_rate * first_buf[m, at, lanes] + second_buf[m, at, lanes]
                gained = (w_buf[m, at, lanes] - learn_rate * hold) * gain
                w_buf[m, at, lanes] = gained
                size = jnp.abs(gained)
                new.append(
                    acc[t] + jnp.sum(size.reshape(STEP // 8, 8, 128), axis=0)
                )
            return tuple(new)

        acc = lax.fori_loop(
            0, rows // STEP, body,
            tuple(jnp.zeros((8, 128), jnp.float32) for _ in range(tiles)),
        )
        for t in range(tiles):
            parts[me, m, :, pl.ds(c + t * 128, 128)] = jnp.sum(
                acc[t], axis=0, keepdims=True
            )

    def send_sums(u):
        m, c, width = units[u]
        at = pl.ds(c, width)
        ref = parts.at[me, m, :, at]
        for peer in peers if u < DIRECT else (diag, x_near, y_near):
            pltpu.make_async_remote_copy(
                src_ref=ref, dst_ref=ref, send_sem=sum_send,
                recv_sem=sum_recv.at[u],
                device_id={"fsdp": peer}, device_id_type=MESH,
            ).start()

    def block(m, owner, first, tall, c, width):
        at = owner * rows + first
        if m == 1:
            at = at + 8 * rows
        if m == 2:
            ref, c = (head, c) if c < head_cols else (tail, c - head_cols)
        else:
            ref = outs
        return block_of(ref, at, tall, c, width)

    def span(tall):
        return outs.at[pl.ds(0, tall), :]

    def send(ref, recv_sem, peer):
        pltpu.make_async_remote_copy(
            src_ref=ref, dst_ref=ref, send_sem=send_sem, recv_sem=recv_sem,
            device_id={"fsdp": peer}, device_id_type=MESH,
        ).start()

    def cross(ref, recv_sem):
        pltpu.make_async_remote_copy(
            src_ref=ref, dst_ref=ref, send_sem=chip_send, recv_sem=recv_sem,
            device_id={"fsdp": partner}, device_id_type=MESH,
        ).start()

    def arrived(ref, recv_sem):
        pltpu.make_async_remote_copy(
            src_ref=ref, dst_ref=ref, send_sem=send_sem, recv_sem=recv_sem,
            device_id={"fsdp": partner}, device_id_type=MESH,
        ).wait_recv()

    def left(ref, sem):
        pltpu.make_async_remote_copy(
            src_ref=ref, dst_ref=ref, send_sem=sem, recv_sem=chip_recv,
            device_id={"fsdp": partner}, device_id_type=MESH,
        ).wait_send()

    def early_copy(side, peer, first, tall):
        at = pl.ds(first, tall)
        return pltpu.make_async_remote_copy(
            src_ref=w_buf.at[0, at, pl.ds(0, early_width)],
            dst_ref=early.at[side, at], send_sem=early_send,
            recv_sem=early_recv.at[side],
            device_id={"fsdp": peer}, device_id_type=MESH,
        )

    def scaled(source, m, owner, lo, hi, c, width):
        scale = jnp.broadcast_to(
            1.0 / factors[m][:, pl.ds(c, width)], (16, width)
        )

        def body(i, carry):
            for k in range(STEP // 16):
                at = pl.multiple_of(i * STEP + k * 16, 16)
                tile = source[pl.ds(at, 16), pl.ds(c, width)] * scale
                block(m, owner, at, 16, c, width)[...] = tile.astype(jnp.bfloat16)
            return carry

        lax.fori_loop(lo // STEP, hi // STEP, body, 0)

    def finish(u):
        m, c, width = units[u]
        at = pl.ds(c, width)
        if u < DIRECT:
            arrived(parts.at[pl.ds(0, 7), m, :, at], sum_recv.at[u])
            total = parts[0, m, :, at]
            for owner in range(1, 8):
                total = total + parts[owner, m, :, at]
        else:
            arrived(parts.at[pl.ds(0, 3), m, :, at], sum_recv.at[u])
            total = parts[core, m, :, at]
            for k in range(1, 4):
                total = total + parts[core + 2 * k, m, :, at]
            pair[core, m, :, at] = total
            ref = pair.at[core, m, :, at]
            pltpu.make_async_remote_copy(
                src_ref=ref, dst_ref=ref, send_sem=sum_send,
                recv_sem=pair_recv.at[u - DIRECT],
                device_id={"fsdp": partner}, device_id_type=MESH,
            ).start()
            arrived(pair.at[0, m, :, at], pair_recv.at[u - DIRECT])
            total = pair[0, m, :, at] + pair[1, m, :, at]
        factors[m][:, at] = total / total_rows
        for h in (1, 0):
            scaled(w_buf.at[m], m, me, h * half, (h + 1) * half, c, width)
            if u == count - 1 or u == 0 and h == 0:
                continue
            ref = block(m, me, h * half, half, c, width)
            send(ref, x_recv.at[m] if h == 0 else x_rest, x_near)
            send(ref, y_recv.at[m] if h == 1 else y_rest, y_near)
        cross(
            block(m, me, 0, rows, c, width),
            chip_tail if u == count - 1 else chip_recv,
        )

    def take_early():
        for side, owner in enumerate((x_near, y_near)):
            arrived(early.at[side], early_recv.at[side])
            scaled(early.at[side], 0, owner, 0, half, 0, early_width)

    sums(0)
    pl.semaphore_wait(barrier, 7)
    send_sums(0)
    early_copy(0, x_near, 0, EARLY).start()
    early_copy(1, y_near, 0, EARLY).start()
    sums(1)
    send_sums(1)
    early_copy(0, x_near, EARLY, half - EARLY).start()
    early_copy(1, y_near, EARLY, half - EARLY).start()
    sums(2)
    send_sums(2)
    finish(0)
    finish(1)
    take_early()
    sums(3)
    send_sums(3)
    finish(2)
    for u in range(4, count):
        sums(u)
        send_sums(u)
    for u in range(3, count):
        finish(u)

    widths = (cols, cols, head_cols)
    pieces = [
        (m, slot, c, width)
        for slot, (m, (c, width)) in enumerate(
            [(0, (0, cols)), (1, (0, cols))] + [(2, run) for run in runs]
        )
    ]
    for m in range(3):
        whole = half * widths[m] // cols
        arrived(span(whole - early_rows * (m == 0)), x_recv.at[m])
        arrived(span(whole), y_recv.at[m])
        for piece, slot, c, width in pieces:
            if piece == m:
                send(
                    block(m, x_near, 0, half, c, width), diag_recv.at[0, slot],
                    y_near,
                )
                send(
                    block(m, y_near, half, half, c, width), diag_recv.at[1, slot],
                    x_near,
                )

    relay = Relay(tail, tail, (x_tail, y_tail, rest_tail, diag_tail), tail_send)

    @pl.when(core == 0)
    def _():
        relay.start()

    arrived(span(2 * half + head_rows // 2), x_rest)
    arrived(span(2 * half + head_rows // 2 - early_rows), y_rest)
    for m in range(3):
        for owner in (x_near, y_near):
            cross(block(m, owner, 0, rows, 0, widths[m]), chip_recv)
    for m, slot, c, width in pieces:
        for h in range(2):
            ref = block(m, diag, h * half, half, c, width)
            arrived(ref, diag_recv.at[h, slot])
            cross(ref, chip_recv)

    @pl.when(core == 0)
    def _():
        for r in range(len(relay.runs)):
            relay.take(r)
            if r < SPLIT:
                relay.forward(r, tail)
        relay.take_rest()
        for r in range(SPLIT):
            relay.finish(r, lambda *at: None)
        relay.left(2, 0, relay.cols)
        relay.left(1, 0, relay.runs[SPLIT][0])

    arrived(span(4 * (2 * rows + head_rows)), chip_recv)
    arrived(tail.at[pl.ds(0, rows), :], chip_tail)
    left(span(3 * (2 * rows + head_rows) - 2 * early_rows), send_sem)
    left(span(4 * (2 * rows + head_rows) + rows - head_rows), chip_send)
    direct = units[DIRECT][1]
    sent = (7 * direct + 4 * (3 * cols - direct)) // 21
    left(parts.at[pl.ds(0, 7), :, :, pl.ds(0, sent)], sum_send)
    left(early, early_send)


def tail_kernel(held, token, value, *sems):
    *relay_sems, relay_send, chip_recv, chip_send, ready = sems
    rows = held.shape[0] // 8
    _, core, partner, x_near, y_near, diag = places()

    barrier = pltpu.get_barrier_semaphore()
    for peer in (x_near, y_near):
        pl.semaphore_signal(
            barrier, inc=1, device_id={"fsdp": peer}, device_id_type=MESH
        )

    @pl.when(core == 1)
    def _():
        pl.semaphore_signal(
            barrier, inc=1, device_id={"fsdp": partner}, device_id_type=MESH
        )

    pl.semaphore_wait(barrier, 3 - core)
    relay = Relay(held, value, relay_sems, relay_send)
    cols = relay.cols
    cut = relay.runs[SPLIT][0]

    def copy_of(source, at, tall, c, width):
        return pltpu.make_async_remote_copy(
            src_ref=block_of(source, at, tall, c, width),
            dst_ref=block_of(value, at, tall, c, width),
            send_sem=chip_send, recv_sem=chip_recv,
            device_id={"fsdp": partner}, device_id_type=MESH,
        )

    @pl.when(core == 0)
    def _():
        pl.semaphore_signal(
            ready, inc=1, device_id={"fsdp": partner}, device_id_type=MESH
        )
        for r in range(SPLIT, len(relay.runs)):
            relay.forward(r, held)
        for owner, width in ((x_near, cols), (y_near, cols), (diag, cut)):
            copy_of(held, owner * rows, rows, 0, width).start()
        for r in range(SPLIT, len(relay.runs)):
            relay.finish(r, lambda *at: copy_of(value, *at).start())
        relay.left(1, cut, cols - cut)

    @pl.when(core == 1)
    def _():
        relay.start()
        for r in range(len(relay.runs)):
            relay.take(r)
            relay.forward(r, value)
        relay.take_rest()
        pl.semaphore_wait(ready, 1)
        for owner in (x_near, y_near):
            copy_of(value, owner * rows, rows, 0, cols).start()
        for r in range(len(relay.runs)):
            relay.finish(r, lambda *at: copy_of(value, *at).start())
        relay.left(3, 0, cols)

    three = copy_of(value, 0, 3 * rows, 0, cols)
    three.wait_recv()
    three.wait_send()


def write_first(src, head, held, *refs):
    lines, outs, line_outs, sem = refs[:3], refs[3:6], refs[6:9], refs[9]
    copies = [
        pltpu.make_async_copy(lines[k], line_outs[k], sem.at[3 + k])
        for k in range(3)
    ]
    for copy in copies:
        copy.start()
    tall = outs[0].shape[0]
    step = tall // PIECES
    width = head.shape[1]
    part = pl.ds(0, width)
    rows = tall // 8
    me, core, *_ = places()
    for p in range(PIECES):
        at = pl.ds(p * step, step)
        for k in range(2):
            pltpu.make_async_copy(
                src.at[pl.ds(k * tall + p * step, step), :], outs[k].at[at, :],
                sem.at[k],
            ).start()
        pltpu.make_async_copy(
            head.at[at, :], outs[2].at[at, part], sem.at[2]
        ).start()
    own = pl.ds(pl.multiple_of((me - core) * rows, 16), 2 * rows)
    rest = pl.ds(width, held.shape[1])
    pair = pltpu.make_async_copy(
        held.at[own, :], outs[2].at[own, rest], sem.at[6]
    )
    pair.start()
    for k in range(2):
        whole = src.at[pl.ds(k * tall, tall), :]
        pltpu.make_async_copy(whole, outs[k], sem.at[k]).wait()
    pair.wait()
    pltpu.make_async_copy(head, outs[2].at[:, part], sem.at[2]).wait()
    for copy in copies:
        copy.wait()


def write_last(held, value, first, out, sem):
    rows = out.shape[0] // 8
    width = held.shape[1]
    start = out.shape[1] - width
    cut = runs_of(TAIL_RUNS, width, sum(TAIL_RUNS))[SPLIT][0]
    _, core, _, x_near, y_near, diag = places()
    step = 8 * rows // PIECES

    def put(src, owner, c=0, wide=width):
        for p in range(rows // step):
            at = owner * rows + p * step
            pltpu.make_async_copy(
                block_of(src, at, step, c, wide),
                block_of(out, at, step, start + c, wide), sem,
            ).start()

    for owner in (x_near, y_near, diag):
        put(value, owner + 1 - 2 * core)

    @pl.when(core == 0)
    def _():
        put(held, x_near)
        put(held, y_near)
        put(held, diag, 0, cut)
        put(value, diag, cut, width - cut)

    @pl.when(core == 1)
    def _():
        for owner in (x_near, y_near, diag):
            put(value, owner)

    six = pl.ds(0, 6 * rows)
    whole = out.at[six, pl.ds(start, width)]
    pltpu.make_async_copy(value.at[six, :], whole, sem).wait()


def ringed(*args, total_rows):
    rows, cols = args[0].shape
    units = units_of(cols)
    count = len(units)
    vmem = pl.BlockSpec(memory_space=pltpu.VMEM)
    hbm = pl.BlockSpec(memory_space=pltpu.HBM)
    dma = pltpu.SemaphoreType.DMA
    tail_cols = units[-1][2]
    head = pltpu.VMEM((8 * rows, cols - tail_cols), jnp.bfloat16)
    tail = pltpu.VMEM((8 * rows, tail_cols), jnp.bfloat16)
    line = jax.ShapeDtypeStruct((1, cols), jnp.float32)
    runs = len(TAIL_RUNS)
    slots = 2 + len(HEAD_RUNS)
    relay = [dma((runs,)), dma((runs,)), dma((2,)), dma((2, runs)), dma]
    pair, head, held, *factors = pl.pallas_call(
        functools.partial(gather_kernel, total_rows),
        out_shape=[pltpu.VMEM((16 * rows, cols), jnp.bfloat16), head, tail]
        + [pltpu.VMEM((1, cols), jnp.float32)] * 3,
        in_specs=[hbm] * 10,
        out_specs=[vmem] * 6,
        scratch_shapes=[
            pltpu.VMEM((3, 3, rows, cols), jnp.float32),
            pltpu.VMEM((1, rows), jnp.float32),
            pltpu.VMEM((rows, 128), jnp.float32),
            pltpu.VMEM((8, 3, 1, cols), jnp.float32),
            pltpu.VMEM((2, 3, 1, cols), jnp.float32),
            pltpu.VMEM((2, rows // 2, units[0][2]), jnp.float32),
            dma((2,)), dma, dma, dma((count,)), dma((count - DIRECT,)), dma, dma((2,)),
            dma((3,)), dma((3,)), dma, dma, dma((2, slots)),
            *relay, dma, dma, dma, dma,
        ],
        compiler_params=pltpu.CompilerParams(
            collective_id=0, has_side_effects=True,
            vmem_limit_bytes=VMEM_BYTES - 3 * 16 * rows * cols - 2**20,
        ),
        name="gather",
    )(*(
        pltpu.with_memory_space_constraint(a, pltpu.HBM)
        for a in (*args[:9], args[9].reshape(1, rows))
    ))
    ready = jax.ShapeDtypeStruct((8 * rows, cols), jnp.bfloat16)
    query, key, first, *lines = pl.pallas_call(
        write_first,
        out_shape=[ready] * 2 + [pltpu.HBM(ready.shape, ready.dtype)] + [line] * 3,
        in_specs=[vmem] * 6,
        out_specs=[hbm] * 6,
        scratch_shapes=[dma((7,))],
        compiler_params=pltpu.CompilerParams(
            has_side_effects=True, vmem_limit_bytes=2**20
        ),
        name="write_first",
    )(pair, head, held, *factors)
    value = pl.pallas_call(
        tail_kernel,
        out_shape=tail,
        in_specs=[vmem, hbm],
        out_specs=vmem,
        scratch_shapes=[*relay, dma, dma, pltpu.SemaphoreType.REGULAR],
        compiler_params=pltpu.CompilerParams(
            collective_id=1, has_side_effects=True, vmem_limit_bytes=2**20
        ),
        name="tail",
    )(held, pltpu.with_memory_space_constraint(lines[0], pltpu.HBM))
    value = pl.pallas_call(
        write_last,
        out_shape=pltpu.HBM(ready.shape, ready.dtype),
        in_specs=[vmem, vmem, hbm],
        out_specs=hbm,
        scratch_shapes=[dma],
        input_output_aliases={2: 0},
        compiler_params=pltpu.CompilerParams(vmem_limit_bytes=2**20),
        name="write_last",
    )(held, value, pltpu.with_memory_space_constraint(first, pltpu.HBM))
    return [query, key, value] + [f.reshape(cols) for f in lines]


def on_device(*args, devices):
    rows, cols = args[0].shape
    total_rows = devices * rows
    fits = rows * cols * (36 + 48) <= 48 * 2**20
    if devices == 8 and rows % 128 == 0 and cols % (128 * UNITS) == 0 and fits:
        return tuple(ringed(*args, total_rows=total_rows))
    return plain(*args, rows=total_rows)


def solution(mesh):
    return jax.shard_map(
        functools.partial(on_device, devices=mesh.shape["fsdp"]),
        mesh=mesh,
        in_specs=(P("fsdp", "model"),) * 9 + (P("fsdp"),),
        out_specs=(P(None, "model"),) * 3 + (P("model"),) * 3,
        check_vma=False,
    )
```

```python
import functools
import math

import jax
import jax.numpy as jnp
from jax import lax
from jax.experimental import pallas as pl
from jax.experimental.pallas import tpu as pltpu
from jax.sharding import PartitionSpec as P

learn_rate = 0.2
hold_rate = 0.9
MESH = pl.DeviceIdType.MESH
UNITS = 8
PARTS = ((1, 2, 5), (8,), (2, 6))
HEAD_RUNS = (2,)
TAIL_RUNS = (2, 2, 1, 1)
DIRECT = 2
EARLY = 96
STEP = 32
AHEAD = 2
PIECES = 32
VMEM_BYTES = 67_043_328


def plain(
    w_query,
    first_query,
    second_query,
    w_key,
    first_key,
    second_key,
    w_value,
    first_value,
    second_value,
    norm_gain,
    rows,
):
    gained = []
    for w, first, second in (
        (w_query, first_query, second_query),
        (w_key, first_key, second_key),
        (w_value, first_value, second_value),
    ):
        hold = hold_rate * first + second
        gained.append((w - learn_rate * hold) * norm_gain[:, None])
    totals = lax.psum(tuple(jnp.sum(jnp.abs(g), axis=0) for g in gained), "fsdp")
    factors = tuple(t / rows for t in totals)
    ready = tuple(
        lax.all_gather(
            (g / f).astype(jnp.bfloat16), "fsdp", axis=0, tiled=True
        )
        for g, f in zip(gained, factors)
    )
    return ready + factors


def units_of(cols):
    units = []
    for m, sizes in enumerate(PARTS):
        first = 0
        for size in sizes:
            units.append((m, first, size * cols // UNITS))
            first += size * cols // UNITS
    return units


def runs_of(sizes, cols, parts):
    runs = []
    first = 0
    for size in sizes:
        runs.append((first, size * cols // parts))
        first += size * cols // parts
    return runs


def places():
    me = lax.axis_index("fsdp")
    core = me % 2
    x = (me // 2) % 2
    y = me // 4
    partner = me + 1 - 2 * core
    x_near = me + 2 - 4 * x
    y_near = me + 4 - 8 * y
    diag = x_near + 4 - 8 * y
    return me, core, partner, x_near, y_near, diag


def block_of(ref, at, tall, c, width):
    return ref.at[pl.ds(pl.multiple_of(at, 16), tall), pl.ds(c, width)]


class Relay:
    def __init__(self, own, far, sems, send_sem):
        self.own, self.far, self.send_sem = own, far, send_sem
        self.x_recv, self.y_recv, self.rest, self.diag_recv = sems
        self.rows = far.shape[0] // 8
        self.half = self.rows // 2
        self.cols = far.shape[1]
        self.me, _, self.partner, self.x_near, self.y_near, self.diag = places()
        self.runs = runs_of(TAIL_RUNS, self.cols, sum(TAIL_RUNS))

    def send(self, source, at, tall, c, width, recv_sem, peer):
        pltpu.make_async_remote_copy(
            src_ref=block_of(source, at, tall, c, width),
            dst_ref=block_of(self.far, at, tall, c, width),
            send_sem=self.send_sem, recv_sem=recv_sem,
            device_id={"fsdp": peer}, device_id_type=MESH,
        ).start()

    def arrived(self, at, tall, c, width, recv_sem):
        ref = block_of(self.far, at, tall, c, width)
        pltpu.make_async_remote_copy(
            src_ref=ref, dst_ref=ref, send_sem=self.send_sem, recv_sem=recv_sem,
            device_id={"fsdp": self.partner}, device_id_type=MESH,
        ).wait_recv()

    def start(self):
        top = self.me * self.rows
        low = top + self.half
        for r, (c, width) in enumerate(self.runs):
            self.send(
                self.own, top, self.half, c, width, self.x_recv.at[r], self.x_near
            )
            self.send(
                self.own, low, self.half, c, width, self.y_recv.at[r], self.y_near
            )
        self.send(
            self.own, low, self.half, 0, self.cols, self.rest.at[0], self.x_near
        )
        self.send(
            self.own, top, self.half, 0, self.cols, self.rest.at[1], self.y_near
        )

    def take(self, r):
        c, width = self.runs[r]
        top = self.x_near * self.rows
        low = self.y_near * self.rows + self.half
        self.arrived(top, self.half, c, width, self.x_recv.at[r])
        self.arrived(low, self.half, c, width, self.y_recv.at[r])

    def forward(self, r, source):
        c, width = self.runs[r]
        top = self.x_near * self.rows
        low = self.y_near * self.rows + self.half
        self.send(
            source, top, self.half, c, width, self.diag_recv.at[0, r], self.y_near
        )
        self.send(
            source, low, self.half, c, width, self.diag_recv.at[1, r], self.x_near
        )

    def take_rest(self):
        for near, first, sem in (
            (self.x_near, self.half, self.rest.at[0]),
            (self.y_near, 0, self.rest.at[1]),
        ):
            self.arrived(near * self.rows + first, self.half, 0, self.cols, sem)

    def finish(self, r, then):
        c, width = self.runs[r]
        for h in range(2):
            at = self.diag * self.rows + h * self.half
            self.arrived(at, self.half, c, width, self.diag_recv.at[h, r])
            then(at, self.half, c, width)

    def left(self, blocks, c, width):
        ref = block_of(self.far, 0, blocks * self.rows, c, width)
        pltpu.make_async_remote_copy(
            src_ref=ref, dst_ref=ref, send_sem=self.send_sem,
            recv_sem=self.x_recv.at[0], device_id={"fsdp": self.partner},
            device_id_type=MESH,
        ).wait_send()


def gather_kernel(total_rows, *refs):
    ins, gain_ref = refs[:9], refs[9]
    outs, head, tail, factors = refs[10], refs[11], refs[12], refs[13:16]
    (
        bufs, gain_line, gain_buf, parts, pair, early,
        load_sem, gain_sem, sum_send, sum_recv, pair_recv, early_send, early_recv,
        x_recv, y_recv, x_rest, y_rest, diag_recv,
        x_tail, y_tail, rest_tail, diag_tail, tail_send,
        chip_recv, chip_tail, send_sem, chip_send,
    ) = refs[16:]
    w_buf, first_buf, second_buf = (bufs.at[k] for k in range(3))
    rows, cols = bufs.shape[2:]
    half = rows // 2

    me, core, partner, x_near, y_near, diag = places()
    peers = [
        diag + 1 - 2 * core, diag, x_near + 1 - 2 * core, y_near + 1 - 2 * core,
        x_near, y_near, partner,
    ]
    units = units_of(cols)
    count = len(units)
    head_cols = head.shape[1]
    runs = runs_of(HEAD_RUNS, head_cols, sum(HEAD_RUNS))
    early_width = units[0][2]
    early_rows = half * early_width // cols
    head_rows = rows * head_cols // cols

    barrier = pltpu.get_barrier_semaphore()
    for peer in peers:
        pl.semaphore_signal(
            barrier, inc=1, device_id={"fsdp": peer}, device_id_type=MESH
        )

    def load(u):
        if u < count:
            m, c, width = units[u]
            at = pl.ds(c, width)
            for k in range(3):
                pltpu.make_async_copy(
                    ins[3 * m + k].at[:, at], bufs.at[k, m, :, at],
                    load_sem.at[u % 2],
                ).start()

    def loaded(u):
        m, c, width = units[u]
        ref = bufs.at[:, m, :, pl.ds(c, width)]
        pltpu.make_async_copy(ref, ref, load_sem.at[u % 2]).wait()

    gain_copy = pltpu.make_async_copy(gain_ref, gain_line, gain_sem)
    gain_copy.start()
    load(0)

    gain_copy.wait()
    load(1)
    for k in range(rows // 128):
        line = gain_line[:, pl.ds(k * 128, 128)]
        gain_buf[pl.ds(k * 128, 128), :] = jnp.broadcast_to(line, (128, 128)).T

    def sums(u):
        m, c, width = units[u]
        loaded(u)
        load(u + AHEAD)
        tiles = width // 128

        def body(i, acc):
            at = pl.ds(pl.multiple_of(i * STEP, STEP), STEP)
            gain = gain_buf[at, :]
            new = []
            for t in range(tiles):
                lanes = pl.ds(c + t * 128, 128)
                hold = hold_rate * first_buf[m, at, lanes] + second_buf[m, at, lanes]
                gained = (w_buf[m, at, lanes] - learn_rate * hold) * gain
                w_buf[m, at, lanes] = gained
                size = jnp.abs(gained)
                new.append(
                    acc[t] + jnp.sum(size.reshape(STEP // 8, 8, 128), axis=0)
                )
            return tuple(new)

        acc = lax.fori_loop(
            0, rows // STEP, body,
            tuple(jnp.zeros((8, 128), jnp.float32) for _ in range(tiles)),
        )
        for t in range(tiles):
            parts[me, m, :, pl.ds(c + t * 128, 128)] = jnp.sum(
                acc[t], axis=0, keepdims=True
            )

    def send_sums(u):
        m, c, width = units[u]
        at = pl.ds(c, width)
        ref = parts.at[me, m, :, at]
        for peer in peers if u < DIRECT else (diag, x_near, y_near):
            pltpu.make_async_remote_copy(
                src_ref=ref, dst_ref=ref, send_sem=sum_send,
                recv_sem=sum_recv.at[u],
                device_id={"fsdp": peer}, device_id_type=MESH,
            ).start()

    def block(m, owner, first, tall, c, width):
        at = owner * rows + first
        if m == 1:
            at = at + 8 * rows
        if m == 2:
            ref, c = (head, c) if c < head_cols else (tail, c - head_cols)
        else:
            ref = outs
        return block_of(ref, at, tall, c, width)

    def span(tall):
        return outs.at[pl.ds(0, tall), :]

    def send(ref, recv_sem, peer):
        pltpu.make_async_remote_copy(
            src_ref=ref, dst_ref=ref, send_sem=send_sem, recv_sem=recv_sem,
            device_id={"fsdp": peer}, device_id_type=MESH,
        ).start()

    def cross(ref, recv_sem):
        pltpu.make_async_remote_copy(
            src_ref=ref, dst_ref=ref, send_sem=chip_send, recv_sem=recv_sem,
            device_id={"fsdp": partner}, device_id_type=MESH,
        ).start()

    def arrived(ref, recv_sem):
        pltpu.make_async_remote_copy(
            src_ref=ref, dst_ref=ref, send_sem=send_sem, recv_sem=recv_sem,
            device_id={"fsdp": partner}, device_id_type=MESH,
        ).wait_recv()

    def left(ref, sem):
        pltpu.make_async_remote_copy(
            src_ref=ref, dst_ref=ref, send_sem=sem, recv_sem=chip_recv,
            device_id={"fsdp": partner}, device_id_type=MESH,
        ).wait_send()

    def early_copy(side, peer, first, tall):
        at = pl.ds(first, tall)
        return pltpu.make_async_remote_copy(
            src_ref=w_buf.at[0, at, pl.ds(0, early_width)],
            dst_ref=early.at[side, at], send_sem=early_send,
            recv_sem=early_recv.at[side],
            device_id={"fsdp": peer}, device_id_type=MESH,
        )

    def scaled(source, m, owner, lo, hi, c, width):
        scale = jnp.broadcast_to(
            1.0 / factors[m][:, pl.ds(c, width)], (16, width)
        )

        def body(i, carry):
            for k in range(STEP // 16):
                at = pl.multiple_of(i * STEP + k * 16, 16)
                tile = source[pl.ds(at, 16), pl.ds(c, width)] * scale
                block(m, owner, at, 16, c, width)[...] = tile.astype(jnp.bfloat16)
            return carry

        lax.fori_loop(lo // STEP, hi // STEP, body, 0)

    def finish(u):
        m, c, width = units[u]
        at = pl.ds(c, width)
        if u < DIRECT:
            arrived(parts.at[pl.ds(0, 7), m, :, at], sum_recv.at[u])
            total = parts[0, m, :, at]
            for owner in range(1, 8):
                total = total + parts[owner, m, :, at]
        else:
            arrived(parts.at[pl.ds(0, 3), m, :, at], sum_recv.at[u])
            total = parts[core, m, :, at]
            for k in range(1, 4):
                total = total + parts[core + 2 * k, m, :, at]
            pair[core, m, :, at] = total
            ref = pair.at[core, m, :, at]
            pltpu.make_async_remote_copy(
                src_ref=ref, dst_ref=ref, send_sem=sum_send,
                recv_sem=pair_recv.at[u - DIRECT],
                device_id={"fsdp": partner}, device_id_type=MESH,
            ).start()
            arrived(pair.at[0, m, :, at], pair_recv.at[u - DIRECT])
            total = pair[0, m, :, at] + pair[1, m, :, at]
        factors[m][:, at] = total / total_rows
        for h in (1, 0):
            scaled(w_buf.at[m], m, me, h * half, (h + 1) * half, c, width)
            if u == count - 1 or u == 0 and h == 0:
                continue
            ref = block(m, me, h * half, half, c, width)
            send(ref, x_recv.at[m] if h == 0 else x_rest, x_near)
            send(ref, y_recv.at[m] if h == 1 else y_rest, y_near)
        cross(
            block(m, me, 0, rows, c, width),
            chip_tail if u == count - 1 else chip_recv,
        )

    def take_early():
        for side, owner in enumerate((x_near, y_near)):
            arrived(early.at[side], early_recv.at[side])
            scaled(early.at[side], 0, owner, 0, half, 0, early_width)

    sums(0)
    pl.semaphore_wait(barrier, 7)
    send_sums(0)
    early_copy(0, x_near, 0, EARLY).start()
    early_copy(1, y_near, 0, EARLY).start()
    sums(1)
    send_sums(1)
    early_copy(0, x_near, EARLY, half - EARLY).start()
    early_copy(1, y_near, EARLY, half - EARLY).start()
    sums(2)
    send_sums(2)
    finish(0)
    finish(1)
    take_early()
    sums(3)
    send_sums(3)
    finish(2)
    for u in range(4, count):
        sums(u)
        send_sums(u)
    for u in range(3, count):
        finish(u)

    widths = (cols, cols, head_cols)
    pieces = [
        (m, slot, c, width)
        for slot, (m, (c, width)) in enumerate(
            [(0, (0, cols)), (1, (0, cols))] + [(2, run) for run in runs]
        )
    ]
    for m in range(3):
        whole = half * widths[m] // cols
        arrived(span(whole - early_rows * (m == 0)), x_recv.at[m])
        arrived(span(whole), y_recv.at[m])
        for piece, slot, c, width in pieces:
            if piece == m:
                send(
                    block(m, x_near, 0, half, c, width), diag_recv.at[0, slot],
                    y_near,
                )
                send(
                    block(m, y_near, half, half, c, width), diag_recv.at[1, slot],
                    x_near,
                )

    relay = Relay(tail, tail, (x_tail, y_tail, rest_tail, diag_tail), tail_send)

    @pl.when(core == 0)
    def _():
        relay.start()

    arrived(span(2 * half + head_rows // 2), x_rest)
    arrived(span(2 * half + head_rows // 2 - early_rows), y_rest)
    for m in range(3):
        for owner in (x_near, y_near):
            cross(block(m, owner, 0, rows, 0, widths[m]), chip_recv)
    for m, slot, c, width in pieces:
        for h in range(2):
            ref = block(m, diag, h * half, half, c, width)
            arrived(ref, diag_recv.at[h, slot])
            cross(ref, chip_recv)

    @pl.when(core == 0)
    def _():
        for r in range(len(relay.runs)):
            relay.take(r)
            relay.forward(r, tail)
        relay.take_rest()
        for r in range(len(relay.runs)):
            relay.finish(r, lambda *at: None)
        relay.left(3, 0, relay.cols)

    arrived(span(4 * (2 * rows + head_rows)), chip_recv)
    arrived(tail.at[pl.ds(0, rows), :], chip_tail)
    left(span(3 * (2 * rows + head_rows) - 2 * early_rows), send_sem)
    left(span(4 * (2 * rows + head_rows) + rows - head_rows), chip_send)
    direct = units[DIRECT][1]
    sent = (7 * direct + 4 * (3 * cols - direct)) // 21
    left(parts.at[pl.ds(0, 7), :, :, pl.ds(0, sent)], sum_send)
    left(early, early_send)


def tail_kernel(held, token, value, *sems):
    *relay_sems, relay_send, chip_recv, chip_send, ready = sems
    rows = held.shape[0] // 8
    _, core, partner, x_near, y_near, diag = places()

    barrier = pltpu.get_barrier_semaphore()
    @pl.when(core == 1)
    def _():
        for peer in (x_near, y_near, partner):
            pl.semaphore_signal(
                barrier, inc=1, device_id={"fsdp": peer}, device_id_type=MESH
            )

    pl.semaphore_wait(barrier, 1 + core)
    relay = Relay(held, value, relay_sems, relay_send)
    cols = relay.cols

    def copy_of(source, at, tall, c, width):
        return pltpu.make_async_remote_copy(
            src_ref=block_of(source, at, tall, c, width),
            dst_ref=block_of(value, at, tall, c, width),
            send_sem=chip_send, recv_sem=chip_recv,
            device_id={"fsdp": partner}, device_id_type=MESH,
        )

    @pl.when(core == 0)
    def _():
        pl.semaphore_signal(
            ready, inc=1, device_id={"fsdp": partner}, device_id_type=MESH
        )
        for owner in (x_near, y_near, diag):
            copy_of(held, owner * rows, rows, 0, cols).start()

    @pl.when(core == 1)
    def _():
        relay.start()
        for r in range(len(relay.runs)):
            relay.take(r)
            relay.forward(r, value)
        relay.take_rest()
        pl.semaphore_wait(ready, 1)
        for owner in (x_near, y_near):
            copy_of(value, owner * rows, rows, 0, cols).start()
        for r in range(len(relay.runs)):
            relay.finish(r, lambda *at: copy_of(value, *at).start())
        relay.left(3, 0, cols)

    three = copy_of(value, 0, 3 * rows, 0, cols)
    three.wait_recv()
    three.wait_send()


def write_first(src, head, held, *refs):
    lines, outs, line_outs, sem = refs[:3], refs[3:6], refs[6:9], refs[9]
    copies = [
        pltpu.make_async_copy(lines[k], line_outs[k], sem.at[3 + k])
        for k in range(3)
    ]
    for copy in copies:
        copy.start()
    tall = outs[0].shape[0]
    step = tall // PIECES
    width = head.shape[1]
    part = pl.ds(0, width)
    rows = tall // 8
    me, core, *_ = places()
    for p in range(PIECES):
        at = pl.ds(p * step, step)
        for k in range(2):
            pltpu.make_async_copy(
                src.at[pl.ds(k * tall + p * step, step), :], outs[k].at[at, :],
                sem.at[k],
            ).start()
        pltpu.make_async_copy(
            head.at[at, :], outs[2].at[at, part], sem.at[2]
        ).start()
    own = pl.ds(pl.multiple_of((me - core) * rows, 16), 2 * rows)
    rest = pl.ds(width, held.shape[1])
    pair = pltpu.make_async_copy(
        held.at[own, :], outs[2].at[own, rest], sem.at[6]
    )
    pair.start()
    for k in range(2):
        whole = src.at[pl.ds(k * tall, tall), :]
        pltpu.make_async_copy(whole, outs[k], sem.at[k]).wait()
    pair.wait()
    pltpu.make_async_copy(head, outs[2].at[:, part], sem.at[2]).wait()
    for copy in copies:
        copy.wait()


def write_last(held, value, first, out, sem):
    rows = out.shape[0] // 8
    width = held.shape[1]
    start = out.shape[1] - width
    _, core, _, x_near, y_near, diag = places()
    step = 8 * rows // PIECES

    def put(src, owner):
        for p in range(rows // step):
            at = owner * rows + p * step
            pltpu.make_async_copy(
                block_of(src, at, step, 0, width),
                block_of(out, at, step, start, width), sem,
            ).start()

    for owner in (x_near, y_near, diag):
        put(value, owner + 1 - 2 * core)

    @pl.when(core == 0)
    def _():
        for owner in (x_near, y_near, diag):
            put(held, owner)

    @pl.when(core == 1)
    def _():
        for owner in (x_near, y_near, diag):
            put(value, owner)

    six = pl.ds(0, 6 * rows)
    whole = out.at[six, pl.ds(start, width)]
    pltpu.make_async_copy(value.at[six, :], whole, sem).wait()


def ringed(*args, total_rows):
    rows, cols = args[0].shape
    units = units_of(cols)
    count = len(units)
    vmem = pl.BlockSpec(memory_space=pltpu.VMEM)
    hbm = pl.BlockSpec(memory_space=pltpu.HBM)
    dma = pltpu.SemaphoreType.DMA
    tail_cols = units[-1][2]
    head = pltpu.VMEM((8 * rows, cols - tail_cols), jnp.bfloat16)
    tail = pltpu.VMEM((8 * rows, tail_cols), jnp.bfloat16)
    line = jax.ShapeDtypeStruct((1, cols), jnp.float32)
    runs = len(TAIL_RUNS)
    slots = 2 + len(HEAD_RUNS)
    relay = [dma((runs,)), dma((runs,)), dma((2,)), dma((2, runs)), dma]
    pair, head, held, *factors = pl.pallas_call(
        functools.partial(gather_kernel, total_rows),
        out_shape=[pltpu.VMEM((16 * rows, cols), jnp.bfloat16), head, tail]
        + [pltpu.VMEM((1, cols), jnp.float32)] * 3,
        in_specs=[hbm] * 10,
        out_specs=[vmem] * 6,
        scratch_shapes=[
            pltpu.VMEM((3, 3, rows, cols), jnp.float32),
            pltpu.VMEM((1, rows), jnp.float32),
            pltpu.VMEM((rows, 128), jnp.float32),
            pltpu.VMEM((8, 3, 1, cols), jnp.float32),
            pltpu.VMEM((2, 3, 1, cols), jnp.float32),
            pltpu.VMEM((2, rows // 2, units[0][2]), jnp.float32),
            dma((2,)), dma, dma, dma((count,)), dma((count - DIRECT,)), dma, dma((2,)),
            dma((3,)), dma((3,)), dma, dma, dma((2, slots)),
            *relay, dma, dma, dma, dma,
        ],
        compiler_params=pltpu.CompilerParams(
            collective_id=0, has_side_effects=True,
            vmem_limit_bytes=VMEM_BYTES - 3 * 16 * rows * cols - 2**20,
        ),
        name="gather",
    )(*(
        pltpu.with_memory_space_constraint(a, pltpu.HBM)
        for a in (*args[:9], args[9].reshape(1, rows))
    ))
    ready = jax.ShapeDtypeStruct((8 * rows, cols), jnp.bfloat16)
    query, key, first, *lines = pl.pallas_call(
        write_first,
        out_shape=[ready] * 2 + [pltpu.HBM(ready.shape, ready.dtype)] + [line] * 3,
        in_specs=[vmem] * 6,
        out_specs=[hbm] * 6,
        scratch_shapes=[dma((7,))],
        compiler_params=pltpu.CompilerParams(
            has_side_effects=True, vmem_limit_bytes=2**20
        ),
        name="write_first",
    )(pair, head, held, *factors)
    value = pl.pallas_call(
        tail_kernel,
        out_shape=tail,
        in_specs=[vmem, hbm],
        out_specs=vmem,
        scratch_shapes=[*relay, dma, dma, pltpu.SemaphoreType.REGULAR],
        compiler_params=pltpu.CompilerParams(
            collective_id=1, has_side_effects=True, vmem_limit_bytes=2**20
        ),
        name="tail",
    )(held, pltpu.with_memory_space_constraint(lines[0], pltpu.HBM))
    value = pl.pallas_call(
        write_last,
        out_shape=pltpu.HBM(ready.shape, ready.dtype),
        in_specs=[vmem, vmem, hbm],
        out_specs=hbm,
        scratch_shapes=[dma],
        input_output_aliases={2: 0},
        compiler_params=pltpu.CompilerParams(vmem_limit_bytes=2**20),
        name="write_last",
    )(held, value, pltpu.with_memory_space_constraint(first, pltpu.HBM))
    return [query, key, value] + [f.reshape(cols) for f in lines]


def on_device(*args, devices):
    rows, cols = args[0].shape
    total_rows = devices * rows
    fits = rows * cols * (36 + 48) <= 48 * 2**20
    if devices == 8 and rows % 128 == 0 and cols % (128 * UNITS) == 0 and fits:
        return tuple(ringed(*args, total_rows=total_rows))
    return plain(*args, rows=total_rows)


def solution(mesh):
    return jax.shard_map(
        functools.partial(on_device, devices=mesh.shape["fsdp"]),
        mesh=mesh,
        in_specs=(P("fsdp", "model"),) * 9 + (P("fsdp"),),
        out_specs=(P(None, "model"),) * 3 + (P("model"),) * 3,
        check_vma=False,
    )
```
